256 devices in a mesh: grp: 8 (over x, core), dev: 32 (over z, y).
Axes of the slice: x: 4, y: 4, z: 8, core: 2. Of those that a mesh axis runs over, the one named last changes fastest.
Arguments:
- points: bfloat16 [524288, 1024], P(('grp', 'dev')), may hold values from -6 to 6
- blocks: int32 [524288, 1], P(('grp', 'dev')), may hold values from 0 to 255; in each aligned block of 2048 rows (0 to 2047, 2048 to 4095, ...) at most 16 rows name the same one
- finals: int32 [524288], P(('grp', 'dev')), may hold values from 0 to 255
- centroids: bfloat16 [65536, 1024], P('dev'), may hold values from -6 to 6
Outputs:
- distances: bfloat16 [524288, 256], P(('grp', 'dev'))
- refreshed_centroids: float32 [65536, 1024], P('dev', 'grp')
The draws below stay inside these ranges and needn't reach their ends.
Inputs may be any that keep to these rules, and one draw needn't show every extreme that they name: `blocks`: among the 2048 rows of one device no block is named by more than 16 rows, and some block by exactly 16. Block b is held by index b // 8 of dev. The point's centroid is row 256 * blocks + finals of centroids.
All inputs are finite; a program needn't handle non-finite values.
Results may differ from the reference program's by a relative error of at most 0.008.
Values may be sent and summed in bfloat16 or wider, within the bound.
A program may use at most 128 MiB of HBM per device.

```python
import math
import jax
import jax.numpy as jnp
import numpy as np
from jax import lax

D = 1024
BS = 256
POINTS_PER_SHARD = 2048
NB = 256
K = 65536
P_SIZE = 524288
MOST = 16
N_GRP = 8
N_DEV = 32


def place_ends(entries, own_key, smallest, top_value):
    dims = entries.shape
    index_at = [jax.random.randint(jax.random.fold_in(own_key, axis), (), 0, dims[axis]) for axis in range(len(dims))]
    entries = entries.at[tuple(index_at)].set(smallest)
    longest = dims.index(max(dims))
    index_at[longest] = (index_at[longest] + 1) % dims[longest]
    return entries.at[tuple(index_at)].set(top_value)


def shard_levels(stream_key, extent, cuts, smallest, top_value):
    def one(position, blocks):
        steps = jax.random.uniform(jax.random.fold_in(jax.random.fold_in(stream_key, 6), position), (blocks,), jnp.float32, smallest / len(cuts), top_value / len(cuts))
        return jnp.repeat(jnp.exp(steps), extent[position] // blocks).reshape((-1,) + (1,) * (len(extent) - position - 1))

    loudness = one(*cuts[0])
    for cut in cuts[1:]:
        loudness = loudness * one(*cut)
    return loudness


def assign_block(key, own, number, rows, count, top, most, skew):
    ranking = jax.random.permutation(key, count)
    heavy_load, usual = load_shares(count, rows * top, most, skew, True), load_shares(count, rows * top, most, skew, False)
    places = jnp.arange(count)

    def named(sizes, offset_by):
        used = int((sizes > 0).sum())
        fixed = max(1, used // 4)
        shifted = fixed + (places - fixed + offset_by * (used - fixed)) % max(1, count - fixed)
        return jnp.zeros((count,), jnp.int32).at[ranking[jnp.where(places < fixed, places, shifted)]].set(jnp.asarray(sizes, jnp.int32))

    sizes = jnp.where(number % 4 == 0, named(heavy_load, number // 4), named(usual, number - number // 4 - 1))
    mixed = jax.random.permutation(jax.random.fold_in(own, 3), count)
    giver, taker = mixed[0:count // 2 * 2:2], mixed[1:count // 2 * 2:2]
    margin = jnp.minimum(sizes[giver] - 1, most - sizes[taker]) // 2
    margin = jnp.where((giver == ranking[0]) | (taker == ranking[0]) | (sizes[taker] == 0), 0, jnp.maximum(margin, 0))
    shifted = jax.random.randint(jax.random.fold_in(own, 4), (count // 2,), 0, 1 << 20) % (margin + 1)
    sizes = sizes.at[giver].add(-shifted).at[taker].add(shifted)
    items = jnp.searchsorted(jnp.cumsum(sizes), jnp.arange(rows * top), side="right").astype(jnp.int32)
    grid = items.reshape(top, rows).T
    grid = grid[jax.random.permutation(jax.random.fold_in(own, 1), rows)]
    offset_by = jax.random.randint(jax.random.fold_in(own, 2), (rows, 1), 0, top)
    return jnp.take_along_axis(grid, (jnp.arange(top)[None, :] + offset_by) % top, axis=1)


def load_shares(amount, total, limit, slope, full):
    loads = [(1 << 20) // math.isqrt(rank ** slope) + 1 for rank in range(1, amount + 1)]
    largest = limit if full else min(limit, max(-(-total // amount), total * loads[0] // sum(loads)))
    least = 1 if total - largest >= amount - 1 else 0
    holding, surplus = [largest] + [least] * (amount - 1), total - largest - least * (amount - 1)
    while surplus > 0:
        free = [i for i in range(1, amount) if holding[i] < largest] or [i for i in range(1, amount) if holding[i] < limit]
        mass, left = sum([loads[i] for i in free]), surplus
        for i in free:
            extra = min(limit - holding[i], max(1, left * loads[i] // mass), surplus)
            holding[i] = holding[i] + extra
            surplus = surplus - extra
    return np.array(holding)


def normal_values(stream_key, dims, scale, bound, pieces=(), held_as=jnp.bfloat16):
    gain = shard_levels(stream_key, dims, pieces, -0.22, 0.18) if pieces else 1.0
    values = jax.random.normal(stream_key, dims, jnp.float32) * scale * gain
    return jnp.minimum(jnp.maximum(values, -bound), bound).astype(held_as)


def setup_inputs(seed: int = 0) -> dict:
    key_list = jax.random.split(jax.random.key(seed), 5)
    points = normal_values(key_list[0], (P_SIZE, D), 1.0, 6.0, ((0, 256),))
    blocks_keys = jax.random.split(jax.random.fold_in(key_list[1], 1), P_SIZE // POINTS_PER_SHARD)
    blocks_turns = jax.random.permutation(jax.random.fold_in(key_list[1], 3), P_SIZE // POINTS_PER_SHARD)
    blocks = jax.vmap(lambda own, number: assign_block(jax.random.fold_in(key_list[1], 2), own, number, POINTS_PER_SHARD, NB, 1, MOST, 2))(blocks_keys, blocks_turns).reshape((P_SIZE, 1))
    finals = place_ends(jax.random.randint(key_list[2], (P_SIZE,), 0, BS), jax.random.fold_in(key_list[2], 1), 0, BS - 1).astype(jnp.int32)
    centroids = normal_values(key_list[3], (K, D), 1.0, 6.0, ((0, 32),))
    return {"points": points, "blocks": blocks, "finals": finals, "centroids": centroids}


def reference(points, blocks, finals, centroids):
    npoints, width = points.shape
    nblocks = centroids.shape[0] // BS
    reach = N_GRP * N_DEV * MOST
    block_ids = blocks[:, 0].astype(jnp.int32)
    order = jnp.argsort(block_ids, stable=True).astype(jnp.int32)
    ordered = block_ids[order]
    labels = jnp.arange(nblocks, dtype=jnp.int32)
    starts = jnp.searchsorted(ordered, labels, side="left").astype(jnp.int32)
    stops = jnp.searchsorted(ordered, labels, side="right").astype(jnp.int32)
    padded = jnp.concatenate([order, jnp.zeros((reach,), jnp.int32)])
    columns = jnp.arange(BS, dtype=jnp.int32)
    positions = jnp.arange(reach, dtype=jnp.int32)

    def one_block(label):
        begin = starts[label]
        chosen = lax.dynamic_slice_in_dim(padded, begin, reach)
        live = positions < (stops[label] - begin)
        rows = points[chosen].astype(jnp.float32)
        centroid_table = lax.dynamic_slice_in_dim(centroids, (label * BS).astype(jnp.int32), BS, 0).astype(jnp.float32)
        cross_products = jnp.dot(rows, centroid_table.T, preferred_element_type=jnp.float32)
        dists = (jnp.sum(rows * rows, axis=1)[:, None] - 2.0 * cross_products + jnp.sum(centroid_table * centroid_table, axis=1)[None, :]) / width
        onehot_assign = jnp.where(live[:, None] & (finals[chosen][:, None] == columns[None, :]), 1.0, 0.0).astype(jnp.float32)
        sums = jnp.dot(onehot_assign.T, rows, preferred_element_type=jnp.float32)
        counts = jnp.sum(onehot_assign, axis=0)
        fresh = (sums + centroid_table) / (counts + 1.0)[:, None]
        where_to = jnp.where(live, chosen, npoints).astype(jnp.int32)
        return dists.astype(jnp.bfloat16), where_to, fresh

    dists, where_to, fresh = lax.map(one_block, labels)
    table = jnp.zeros((npoints + 1, BS), jnp.bfloat16).at[where_to.reshape(-1)].set(dists.reshape(-1, BS))
    return table[:npoints], fresh.reshape(nblocks * BS, width)
```

```python
import jax
import jax.numpy as jnp
from jax import lax
from jax.sharding import Mesh, PartitionSpec as P

BS = 256
NZ = 8
SLAB = ("x", "core", "y")


def shards(points, blocks, finals, centroids):
    npoints, width = points.shape
    owned = centroids.shape[0] // BS
    ny = lax.axis_size("y")
    nblocks = owned * NZ * ny
    depth = 2 * npoints // nblocks
    g = lax.axis_index(("x", "core"))
    own_block = lax.dynamic_slice_in_dim(centroids, g * BS, BS, 0)
    table = lax.all_gather(own_block, "z", axis=0, tiled=False)

    block_ids = blocks[:, 0]
    dest = ((block_ids % owned) * ny + (block_ids // owned) % ny) * NZ + block_ids // (owned * ny)
    labels = jnp.arange(nblocks, dtype=jnp.int32)
    member = dest[:, None] == labels[None, :]
    lower = (jnp.arange(npoints)[:, None] > jnp.arange(npoints)[None, :]).astype(jnp.bfloat16)
    before = jnp.dot(lower, member.astype(jnp.bfloat16), preferred_element_type=jnp.float32)
    ranks = jnp.sum(jnp.where(member, before, 0.0), axis=1).astype(jnp.int32)
    slots = dest * depth + ranks
    outgoing = jnp.zeros((nblocks * depth, width), jnp.bfloat16).at[slots].set(points)
    targets = jnp.full((nblocks * depth,), -1, jnp.int32).at[slots].set(finals)
    outgoing = outgoing.reshape(nblocks, depth, width)
    targets = targets.reshape(nblocks, depth)
    received = lax.all_to_all(outgoing, SLAB, split_axis=0, concat_axis=1, tiled=True)
    wanted = lax.all_to_all(targets, SLAB, split_axis=0, concat_axis=1, tiled=True)

    cent_norm = jnp.sum(jnp.square(table.astype(jnp.float32)), axis=-1)
    row_norm = jnp.sum(jnp.square(received.astype(jnp.float32)), axis=-1)
    cross = jnp.einsum("nzy,nvy->nzv", received, table, preferred_element_type=jnp.float32)
    dists = ((row_norm[:, :, None] - 2.0 * cross + cent_norm[:, None, :]) / width).astype(jnp.bfloat16)
    onehot = wanted[:, :, None] == jnp.arange(BS, dtype=jnp.int32)[None, None, :]
    sums = jnp.einsum("xnt,xni->xti", onehot.astype(jnp.bfloat16), received, preferred_element_type=jnp.float32)
    counts = jnp.sum(onehot.astype(jnp.float32), axis=1)
    returned = lax.all_to_all(dists, SLAB, split_axis=1, concat_axis=0, tiled=True)
    distances = returned.reshape(nblocks * depth, BS)[slots]
    own_sums = lax.psum_scatter(sums.astype(jnp.bfloat16), "z", scatter_dimension=0, tiled=True)
    own_sums = own_sums.reshape(BS, width).astype(jnp.float32)
    own_counts = lax.psum_scatter(counts, "z", scatter_dimension=0, tiled=True).reshape(BS)
    fresh = (own_sums + own_block.astype(jnp.float32)) / (own_counts + 1.0)[:, None]
    refreshed = lax.all_to_all(
        fresh.astype(jnp.bfloat16), ("x", "core"), split_axis=1, concat_axis=0, tiled=True
    ).astype(jnp.float32)
    return distances, refreshed


def solution(mesh):
    ngrp, ndev = mesh.shape["grp"], mesh.shape["dev"]
    fine = Mesh(mesh.devices.reshape(ngrp // 2, 2, NZ, ndev // NZ), ("x", "core", "z", "y"))
    rows = ("x", "core", "z", "y")
    return jax.shard_map(
        shards,
        mesh=fine,
        in_specs=(P(rows, None), P(rows, None), P(rows), P(("z", "y"), None)),
        out_specs=(P(rows, None), P(("z", "y"), ("x", "core"))),
        check_vma=False,
    )
```

```python
import jax
import jax.numpy as jnp
from jax import lax
from jax.sharding import Mesh, PartitionSpec as P

BS = 256
NZ = 8
SLAB = ("x", "core", "y")


def shards(points, blocks, finals, centroids):
    npoints, width = points.shape
    owned = centroids.shape[0] // BS
    ny = lax.axis_size("y")
    nblocks = owned * NZ * ny
    depth = 2 * npoints // nblocks
    g = lax.axis_index(("x", "core"))
    own_block = lax.dynamic_slice_in_dim(centroids, g * BS, BS, 0)
    table = lax.all_gather(own_block, "z", axis=0, tiled=False)

    block_ids = blocks[:, 0]
    dest = ((block_ids % owned) * ny + (block_ids // owned) % ny) * NZ + block_ids // (owned * ny)
    labels = jnp.arange(nblocks, dtype=jnp.int32)
    member = dest[:, None] == labels[None, :]
    lower = (jnp.arange(npoints)[:, None] > jnp.arange(npoints)[None, :]).astype(jnp.bfloat16)
    before = jnp.dot(lower, member.astype(jnp.bfloat16), preferred_element_type=jnp.float32)
    ranks = jnp.sum(jnp.where(member, before, 0.0), axis=1).astype(jnp.int32)
    slots = dest * depth + ranks
    outgoing = jnp.zeros((nblocks * depth, width), jnp.bfloat16).at[slots].set(points)
    targets = jnp.full((nblocks * depth,), -1, jnp.int32).at[slots].set(finals)
    outgoing = outgoing.reshape(nblocks, depth, width)
    targets = targets.reshape(nblocks, depth)
    outgoing, table = lax.optimization_barrier((outgoing, table))
    received = lax.all_to_all(outgoing, SLAB, split_axis=0, concat_axis=1, tiled=True)
    wanted = lax.all_to_all(targets, SLAB, split_axis=0, concat_axis=1, tiled=True)

    cent_norm = jnp.sum(jnp.square(table.astype(jnp.float32)), axis=-1)
    row_norm = jnp.sum(jnp.square(received.astype(jnp.float32)), axis=-1)
    cross = jnp.einsum("nzy,nvy->nzv", received, table, preferred_element_type=jnp.float32)
    dists = ((row_norm[:, :, None] - 2.0 * cross + cent_norm[:, None, :]) / width).astype(jnp.bfloat16)
    onehot = wanted[:, :, None] == jnp.arange(BS, dtype=jnp.int32)[None, None, :]
    sums = jnp.einsum("xnt,xni->xti", onehot.astype(jnp.bfloat16), received, preferred_element_type=jnp.float32)
    counts = jnp.sum(onehot.astype(jnp.float32), axis=1)
    returned = lax.all_to_all(dists, SLAB, split_axis=1, concat_axis=0, tiled=True)
    distances = returned.reshape(nblocks * depth, BS)[slots]
    own_sums = lax.psum_scatter(sums.astype(jnp.bfloat16), "z", scatter_dimension=0, tiled=True)
    own_sums = own_sums.reshape(BS, width).astype(jnp.float32)
    own_counts = lax.psum_scatter(counts, "z", scatter_dimension=0, tiled=True).reshape(BS)
    fresh = (own_sums + own_block.astype(jnp.float32)) / (own_counts + 1.0)[:, None]
    refreshed = lax.all_to_all(
        fresh.astype(jnp.bfloat16), ("x", "core"), split_axis=1, concat_axis=0, tiled=True
    ).astype(jnp.float32)
    return distances, refreshed


def solution(mesh):
    ngrp, ndev = mesh.shape["grp"], mesh.shape["dev"]
    fine = Mesh(mesh.devices.reshape(ngrp // 2, 2, NZ, ndev // NZ), ("x", "core", "z", "y"))
    rows = ("x", "core", "z", "y")
    return jax.shard_map(
        shards,
        mesh=fine,
        in_specs=(P(rows, None), P(rows, None), P(rows), P(("z", "y"), None)),
        out_specs=(P(rows, None), P(("z", "y"), ("x", "core"))),
        check_vma=False,
    )
```

```python
import functools

import jax
import jax.numpy as jnp
from jax import lax
from jax.experimental import pallas as pl
from jax.experimental.pallas import tpu as pltpu
from jax.sharding import Mesh, PartitionSpec as P

BS = 256
NZ = 8
PIECES = 2
DEPTH = 16
MESH = pl.DeviceIdType.MESH
F32, BF16 = jnp.float32, jnp.bfloat16
NT = (((1,), (1,)), ((), ()))


def kernel(
    dims, slots_row, slots_col, finals_row, points, centroids, dist_out, fresh_out,
    sendbuf, recvbuf, table, sums, partial, dsend, dret, rsend, rrecv, tsend, trecv, tall,
    csend, crecv, cnorm, denom, fsend, frecv, acc,
    p_send, p_recv, t_send, t_recv, d_send, d_recv, g_send, g_recv, r_send, r_recv,
    c_send, c_recv, f_send, f_recv, local_sem,
):
    nx, nc, ny = dims
    ng = nx * nc
    slab = ng * ny
    x, c, z, y = (lax.axis_index(a) for a in ("x", "core", "z", "y"))
    g = x * nc + c
    me = g * ny + y
    npoints, width = points.shape
    cols = width // PIECES
    chunk = NZ * DEPTH
    nrow = slab * DEPTH
    per = 128 // DEPTH

    def at(d):
        g2 = d // ny
        return (g2 // nc, g2 % nc, z, d % ny)

    def along(step):
        return (x, c, (z + step + NZ) % NZ, y)

    def remote(src, dst, ssem, rsem, dev):
        return pltpu.make_async_remote_copy(
            src_ref=src, dst_ref=dst, send_sem=ssem, recv_sem=rsem, device_id=dev, device_id_type=MESH
        )

    def point_copy(h, d, slot):
        return remote(sendbuf.at[h, d], recvbuf.at[h, slot], p_send.at[h, d], p_recv.at[h, slot], at(d))

    def target_copy(d, slot):
        return remote(tsend.at[d], trecv.at[slot], t_send.at[d], t_recv.at[slot], at(d))

    def dist_copy(d, slot):
        return remote(dsend.at[d], dret.at[slot], d_send.at[d], d_recv.at[slot], at(d))

    def count_copy(z2, slot):
        return remote(csend.at[z2], crecv.at[slot], c_send.at[z2], c_recv.at[slot], (x, c, z2, y))

    def fresh_copy(g2, slot):
        return remote(fsend.at[g2], frecv.at[slot], f_send.at[g2], f_recv.at[slot], (g2 // nc, g2 % nc, z, y))

    def others(n, own, fn):
        def body(i, _):
            @pl.when(i != own)
            def _():
                fn(i)

            return 0

        lax.fori_loop(0, n, body, 0)

    barrier = pltpu.get_barrier_semaphore()
    others(slab, me, lambda d: pl.semaphore_signal(barrier, inc=1, device_id=at(d), device_id_type=MESH))
    others(
        NZ, z, lambda z2: pl.semaphore_signal(barrier, inc=1, device_id=(x, c, z2, y), device_id_type=MESH)
    )
    own_copy = pltpu.make_async_copy(
        centroids.at[pl.ds(pl.multiple_of(g * BS, BS), BS)], table.at[z], local_sem
    )
    own_copy.start()

    slots = slots_row[...]
    dest = lax.shift_right_logical(slots, 4)
    rank = slots - dest * DEPTH
    value = (finals_row[...] + 1).astype(F32)
    which = lax.broadcasted_iota(jnp.int32, (slab * NZ, npoints), 0) == dest
    place = lax.broadcasted_iota(jnp.int32, (128, npoints), 0) == rank + (me % per) * DEPTH
    tiles = lax.dot_general(
        jnp.where(which, value, 0.0).astype(BF16), jnp.where(place, 1.0, 0.0).astype(BF16), NT,
        preferred_element_type=F32,
    )
    tsend[...] = tiles.reshape(slab, NZ, 128)
    trecv[me] = tsend[me]
    own_copy.wait()
    pl.semaphore_wait(barrier, slab - 1 + NZ - 1)
    others(slab, me, lambda d: target_copy(d, me).start())

    def ring_copy(way, step, back):
        step_z = 1 if way == 0 else -1
        owner = (z - step_z * (step - back) + 2 * NZ) % NZ if not back else (z - step_z * (step + 1) + 2 * NZ) % NZ
        rows = slice(None) if step < 3 else pl.ds(way * (BS // 2), BS // 2)
        ref = table.at[owner, rows] if step == 3 else table.at[owner]
        return remote(ref, ref, g_send.at[way, step], g_recv.at[way, step], along(step_z))

    def ring_step(step):
        for way in range(2):
            if step:
                ring_copy(way, step - 1, 1).wait_recv()
            if step < 4:
                ring_copy(way, step, 0).start()

    ring_step(0)

    def dispatch(h):
        def body(i, _):
            turn = (2 * (i % nx) + 1) % 5 if nx == 4 else i % nx
            g2 = ((x + turn) % nx) * nc + (c + i // nx) % nc
            hot = lax.broadcasted_iota(jnp.int32, (ny * chunk, npoints), 0) + g2 * (ny * chunk) == slots_row[...]
            moved = jnp.dot(
                jnp.where(hot, 1.0, 0.0).astype(BF16), points[:, h * cols : (h + 1) * cols],
                preferred_element_type=F32,
            ).astype(BF16)
            sendbuf[h, pl.ds(g2 * ny, ny)] = moved.reshape(ny, chunk, cols)
            for dy in range(ny):
                d = g2 * ny + (y + dy) % ny

                @pl.when(d != me)
                def _():
                    point_copy(h, d, me).start()

            return 0

        lax.fori_loop(0, ng, body, 0)
        recvbuf[h, me] = sendbuf[h, me]

    for h in range(PIECES):
        dispatch(h)
        ring_step(h + 1)
    for step in range(PIECES + 1, 5):
        ring_step(step)

    others(slab, me, lambda s: target_copy(s, s).wait_recv())
    for q in range(max(1, slab // per)):
        tile = trecv[q * per]
        for s in range(q * per + 1, min(slab, (q + 1) * per)):
            tile = tile + trecv[s]
        tall[:, q * 128 : (q + 1) * 128] = tile

    def norms(j, _):
        block = table[j].astype(F32)
        column = jnp.sum(block * block, axis=1, keepdims=True)
        cnorm[j] = jnp.broadcast_to(column, (BS, 128)).T[:8]
        return 0

    lax.fori_loop(0, NZ, norms, 0)

    def rows_of(h, j):
        return recvbuf[h, :, pl.ds(pl.multiple_of(j * DEPTH, DEPTH), DEPTH), :].reshape(nrow, cols)

    def add_up(h):
        def body(j, _):
            want = tall[pl.ds(j, 1), :][:, :nrow]
            centroid = lax.broadcasted_iota(jnp.int32, (BS, nrow), 0).astype(F32) + 1.0
            hot = jnp.where(want == centroid, 1.0, 0.0).astype(BF16)
            sums[j, :, h * cols : (h + 1) * cols] = jnp.dot(hot, rows_of(h, j), preferred_element_type=F32)
            if h == 0:
                csend[j] = lax.dot_general(jnp.ones((8, nrow), BF16), hot, NT, preferred_element_type=F32)
            return 0

        lax.fori_loop(0, NZ, body, 0)

    def measure(h):
        def body(j, _):
            rows = rows_of(h, j)
            wide = rows.astype(F32)
            cross = lax.dot_general(
                rows, table[j, :, h * cols : (h + 1) * cols], NT, preferred_element_type=F32
            )
            part = jnp.sum(wide * wide, axis=1, keepdims=True) - 2.0 * cross
            if h > 0:
                part = part + partial[j]
            if h < PIECES - 1:
                partial[j] = part
            else:
                whole = (part + cnorm[j, :1, :]) / width
                dsend[:, pl.ds(pl.multiple_of(j * DEPTH, DEPTH), DEPTH), :] = whole.astype(BF16).reshape(
                    slab, DEPTH, BS
                )
            return 0

        lax.fori_loop(0, NZ, body, 0)

    half = BS // 2

    def reduce_copy(h, way, step):
        rows = pl.ds(way * half, half)
        src = rsend.at[h, way, step, rows] if step == 0 else rsend.at[h, way, step]
        dst = rrecv.at[h, way, step, rows] if step == 0 else rrecv.at[h, way, step]
        return remote(src, dst, r_send.at[h, way, step], r_recv.at[h, way, step], along(1 if way == 0 else -1))

    def reduce_step(h, step):
        piece = slice(h * cols, (h + 1) * cols)
        for way in range(2):
            lo, hi = way * half, (way + 1) * half
            if step == 0:
                rsend[h, way, 0, lo:hi] = sums[(z + 4) % NZ, lo:hi, piece].astype(BF16)
            else:
                target = (z + 4 - step) % NZ if way == 0 else (z + 4 + step) % NZ
                reduce_copy(h, way, step - 1).wait_recv()
                if step == 1:
                    olo, ohi = (1 - way) * half, (2 - way) * half
                    rsend[h, way, 1, lo:hi] = (
                        sums[target, lo:hi, piece] + rrecv[h, way, 0, lo:hi].astype(F32)
                    ).astype(BF16)
                    rsend[h, way, 1, olo:ohi] = sums[target, olo:ohi, piece].astype(BF16)
                else:
                    rsend[h, way, step] = (
                        sums[target, :, piece] + rrecv[h, way, step - 1].astype(F32)
                    ).astype(BF16)
            reduce_copy(h, way, step).start()

    def finish(h):
        piece = slice(h * cols, (h + 1) * cols)
        for way in range(2):
            reduce_copy(h, way, 3).wait_recv()
        if h == 0:
            others(NZ, z, lambda z2: count_copy(z2, z2).wait_recv())
            total = csend[z]
            crecv[z] = total
            total = crecv[0]
            for z2 in range(1, NZ):
                total = total + crecv[z2]
            denom[...] = jnp.broadcast_to(total[:1], (128, BS)).T + 1.0
        own = (
            sums[z, :, piece] + rrecv[h, 0, 3].astype(F32) + rrecv[h, 1, 3].astype(F32)
            + table[z, :, piece].astype(F32)
        )
        share = width // ng
        for q in range(cols // share):
            g2 = h * (cols // share) + q
            fsend[g2] = (own[:, q * share : (q + 1) * share] / denom[:, :share]).astype(BF16)

            @pl.when(g2 != g)
            def _():
                fresh_copy(g2, g).start()

    for h in range(PIECES):
        others(slab, me, lambda s: point_copy(h, s, s).wait_recv())
        add_up(h)
        if h == 0:
            others(NZ, z, lambda z2: count_copy(z2, z).start())
        reduce_step(h, 0)
        measure(h)
        if h == PIECES - 1:
            others(slab, me, lambda d: dist_copy(d, me).start())
            dret[me] = dsend[me]
        for step in range(1, 4):
            reduce_step(h, step)
        finish(h)

    def bring(i, _):
        turn = (2 * (i % nx) + 1) % 5 if nx == 4 else i % nx
        g2 = ((x + turn) % nx) * nc + (c + i // nx) % nc
        for dy in range(ny):
            d = g2 * ny + dy

            @pl.when(d != me)
            def _():
                dist_copy(d, d).wait_recv()

        hot = lax.broadcasted_iota(jnp.int32, (npoints, ny * chunk), 1) + g2 * (ny * chunk) == slots_col[...]
        part = jnp.dot(
            jnp.where(hot, 1.0, 0.0).astype(BF16), dret[pl.ds(g2 * ny, ny)].reshape(ny * chunk, BS),
            preferred_element_type=F32,
        )

        @pl.when(i == 0)
        def _():
            acc[...] = part

        @pl.when(i > 0)
        def _():
            acc[...] += part

        return 0

    lax.fori_loop(0, ng, bring, 0)
    dist_out[...] = acc[...].astype(BF16)

    others(ng, g, lambda g2: fresh_copy(g2, g2).wait_recv())
    frecv[g] = fsend[g]
    for g2 in range(ng):
        fresh_out[g2 * BS : (g2 + 1) * BS, :] = frecv[g2].astype(F32)

    others(slab, me, lambda d: target_copy(d, me).wait_send())
    others(slab, me, lambda d: dist_copy(d, me).wait_send())
    others(NZ, z, lambda z2: count_copy(z2, z).wait_send())
    others(ng, g, lambda g2: fresh_copy(g2, g).wait_send())
    for way in range(2):
        for step in range(4):
            ring_copy(way, step, 0).wait_send()
    for h in range(PIECES):
        others(slab, me, lambda d: point_copy(h, d, me).wait_send())
        for way in range(2):
            for step in range(4):
                reduce_copy(h, way, step).wait_send()


def fused(slots, finals, points, centroids, dims):
    nx, nc, ny = dims
    ng, slab = nx * nc, nx * nc * ny
    npoints, width = points.shape
    cols, chunk, share = width // PIECES, NZ * DEPTH, width // (nx * nc)
    vmem, dma = pltpu.VMEM, pltpu.SemaphoreType.DMA
    tall_lanes = max(1, slab * DEPTH // 128) * 128
    return pl.pallas_call(
        functools.partial(kernel, dims),
        out_shape=(
            jax.ShapeDtypeStruct((npoints, BS), BF16),
            jax.ShapeDtypeStruct((ng * BS, share), F32),
        ),
        in_specs=[pl.BlockSpec(memory_space=vmem)] * 4 + [pl.BlockSpec(memory_space=pl.ANY)],
        out_specs=(pl.BlockSpec(memory_space=vmem),) * 2,
        scratch_shapes=[
            vmem((PIECES, slab, chunk, cols), BF16),
            vmem((PIECES, slab, chunk, cols), BF16),
            vmem((NZ, BS, width), BF16),
            vmem((NZ, BS, width), F32),
            vmem((NZ, slab * DEPTH, BS), F32),
            vmem((slab, chunk, BS), BF16),
            vmem((slab, chunk, BS), BF16),
            vmem((PIECES, 2, 4, BS, cols), BF16),
            vmem((PIECES, 2, 4, BS, cols), BF16),
            vmem((slab, NZ, 128), F32),
            vmem((slab, NZ, 128), F32),
            vmem((NZ, tall_lanes), F32),
            vmem((NZ, 8, BS), F32),
            vmem((NZ, 8, BS), F32),
            vmem((NZ, 8, BS), F32),
            vmem((BS, 128), F32),
            vmem((ng, BS, share), BF16),
            vmem((ng, BS, share), BF16),
            vmem((npoints, BS), F32),
            dma((PIECES, slab)), dma((PIECES, slab)), dma((slab,)), dma((slab,)), dma((slab,)), dma((slab,)),
            dma((2, 4)), dma((2, 4)), dma((PIECES, 2, 4)), dma((PIECES, 2, 4)),
            dma((NZ,)), dma((NZ,)), dma((ng,)), dma((ng,)), dma,
        ],
        compiler_params=pltpu.CompilerParams(
            collective_id=0, has_side_effects=True, vmem_limit_bytes=67043328
        ),
    )(slots[None, :], slots[:, None], finals[None, :], points, centroids)


def shards(points, blocks, finals, centroids):
    npoints, width = points.shape
    owned = centroids.shape[0] // BS
    dims = tuple(lax.axis_size(a) for a in ("x", "core", "y"))
    ny = dims[2]
    nblocks = owned * NZ * ny
    block_ids = blocks[:, 0]
    dest = ((block_ids % owned) * ny + (block_ids // owned) % ny) * NZ + block_ids // (owned * ny)
    labels = jnp.arange(nblocks, dtype=jnp.int32)
    member = dest[:, None] == labels[None, :]
    lower = (jnp.arange(npoints)[:, None] > jnp.arange(npoints)[None, :]).astype(BF16)
    before = jnp.dot(lower, member.astype(BF16), preferred_element_type=F32)
    ranks = jnp.sum(jnp.where(member, before, 0.0), axis=1).astype(jnp.int32)
    slots = dest * DEPTH + ranks
    return fused(slots, finals, points, centroids, dims)


def solution(mesh):
    ngrp, ndev = mesh.shape["grp"], mesh.shape["dev"]
    fine = Mesh(mesh.devices.reshape(ngrp // 2, 2, NZ, ndev // NZ), ("x", "core", "z", "y"))
    rows = ("x", "core", "z", "y")
    return jax.shard_map(
        shards,
        mesh=fine,
        in_specs=(P(rows, None), P(rows, None), P(rows), P(("z", "y"), None)),
        out_specs=(P(rows, None), P(("z", "y"), ("x", "core"))),
        check_vma=False,
    )
```

```python
import functools

import jax
import jax.numpy as jnp
from jax import lax
from jax.experimental import pallas as pl
from jax.experimental.pallas import tpu as pltpu
from jax.sharding import Mesh, PartitionSpec as P

BS = 256
NZ = 8
SPLIT = (4, 2, 2)
DEPTH = 16
MESH = pl.DeviceIdType.MESH
F32, BF16 = jnp.float32, jnp.bfloat16
NT = (((1,), (1,)), ((), ()))


def kernel(
    dims, blocks_row, finals_row, points, centroids, dist_out, fresh_out,
    sendbuf, recvbuf, rsend, rrecv, table, sums, partial, dsend, dret, tsend, trecv, tall,
    csend, crecv, cnorm, denom, fsend, acc, slots_row, slots_col,
    p_send, p_recv, t_send, t_recv, d_send, d_recv, g_send, g_recv, r_send, r_recv,
    c_send, c_recv, f_send, f_recv, local_sem,
):
    nx, nc, ny = dims
    ng = nx * nc
    slab = ng * ny
    x, c, z, y = (lax.axis_index(a) for a in ("x", "core", "z", "y"))
    g = x * nc + c
    me = g * ny + y
    npoints, width = points.shape
    pieces = [slice(a, b) for a, b in bounds(width)]
    frecv = fresh_out
    chunk = NZ * DEPTH
    nrow = slab * DEPTH
    per = 128 // DEPTH

    def at(d):
        g2 = d // ny
        return (g2 // nc, g2 % nc, z, d % ny)

    def along(step):
        return (x, c, (z + step + NZ) % NZ, y)

    def remote(src, dst, ssem, rsem, dev):
        return pltpu.make_async_remote_copy(
            src_ref=src, dst_ref=dst, send_sem=ssem, recv_sem=rsem, device_id=dev, device_id_type=MESH
        )

    def point_copy(h, d, slot):
        return remote(sendbuf[h].at[d], recvbuf[h].at[slot], p_send.at[h, d], p_recv.at[h, slot], at(d))

    def target_copy(d, slot):
        return remote(tsend.at[d], trecv.at[slot], t_send.at[d], t_recv.at[slot], at(d))

    def dist_copy(d, slot):
        return remote(dsend.at[d], dret.at[slot], d_send.at[d], d_recv.at[slot], at(d))

    def count_copy(z2, slot):
        return remote(csend.at[z2], crecv.at[slot], c_send.at[z2], c_recv.at[slot], (x, c, z2, y))

    def fresh_copy(g2, slot):
        return remote(fsend.at[g2], frecv.at[slot], f_send.at[g2], f_recv.at[slot], (g2 // nc, g2 % nc, z, y))

    def others(n, own, fn):
        def body(i, _):
            @pl.when(i != own)
            def _():
                fn(i)

            return 0

        lax.fori_loop(0, n, body, 0)

    def offset(i):
        turn = (2 * (i % nx) + 1) % 5 if nx == 4 else i % nx
        return turn, i // nx

    barrier = pltpu.get_barrier_semaphore()
    others(slab, me, lambda d: pl.semaphore_signal(barrier, inc=1, device_id=at(d), device_id_type=MESH))
    others(
        NZ, z, lambda z2: pl.semaphore_signal(barrier, inc=1, device_id=(x, c, z2, y), device_id_type=MESH)
    )
    own_copy = pltpu.make_async_copy(
        centroids.at[pl.ds(pl.multiple_of(g * BS, BS), BS)], table.at[z], local_sem
    )
    own_copy.start()

    ids = blocks_row[...]
    dest = ((ids & (ng - 1)) * ny + (lax.shift_right_logical(ids, ng.bit_length() - 1) & (ny - 1))) * NZ
    dest = dest + lax.shift_right_logical(ids, (ng * ny).bit_length() - 1)
    strip = min(256, npoints)
    earlier = lax.broadcasted_iota(jnp.int32, (strip, strip), 0) < lax.broadcasted_iota(jnp.int32, (strip, strip), 1)
    earlier = jnp.where(earlier, 1.0, 0.0).astype(BF16)
    seen = jnp.zeros((slab * NZ, 1), F32)
    ranks = []
    for q in range(npoints // strip):
        part = dest[:, q * strip : (q + 1) * strip]
        member = jnp.where(lax.broadcasted_iota(jnp.int32, (slab * NZ, strip), 0) == part, 1.0, 0.0)
        before = jnp.dot(member.astype(BF16), earlier, preferred_element_type=F32) + seen
        ranks.append(jnp.sum(member * before, axis=0, keepdims=True))
        seen = seen + jnp.sum(member, axis=1, keepdims=True)
    rank = jnp.concatenate(ranks, axis=1).astype(jnp.int32)
    slots = dest * DEPTH + rank
    slots_row[...] = slots
    slots_col[...] = jnp.broadcast_to(slots.astype(F32), (128, npoints)).T.astype(jnp.int32)

    value = (finals_row[...] + 1).astype(F32)
    which = lax.broadcasted_iota(jnp.int32, (slab * NZ, npoints), 0) == dest
    place = lax.broadcasted_iota(jnp.int32, (128, npoints), 0) == rank + (me % per) * DEPTH
    tiles = lax.dot_general(
        jnp.where(which, value, 0.0).astype(BF16), jnp.where(place, 1.0, 0.0).astype(BF16), NT,
        preferred_element_type=F32,
    )
    tsend[...] = tiles.reshape(slab, NZ, 128)
    trecv[me] = tsend[me]
    own_copy.wait()
    pl.semaphore_wait(barrier, slab - 1 + NZ - 1)
    others(slab, me, lambda d: target_copy(d, me).start())

    def ring_copy(way, step, back):
        step_z = 1 if way == 0 else -1
        owner = (z - step_z * (step - back) + 2 * NZ) % NZ if not back else (z - step_z * (step + 1) + 2 * NZ) % NZ
        rows = slice(None) if step < 3 else pl.ds(way * (BS // 2), BS // 2)
        ref = table.at[owner, rows] if step == 3 else table.at[owner]
        return remote(ref, ref, g_send.at[way, step], g_recv.at[way, step], along(step_z))

    def ring_step(step):
        for way in range(2):
            if step:
                ring_copy(way, step - 1, 1).wait_recv()
            if step < 4:
                ring_copy(way, step, 0).start()

    ring_step(0)

    def dispatch(h):
        def body(i, _):
            dx, dc = offset(i)
            g2 = ((x + dx) % nx) * nc + (c + dc) % nc
            hot = lax.broadcasted_iota(jnp.int32, (ny * chunk, npoints), 0) + g2 * (ny * chunk) == slots_row[...]
            moved = jnp.dot(
                jnp.where(hot, 1.0, 0.0).astype(BF16), points[:, pieces[h]],
                preferred_element_type=F32,
            ).astype(BF16)
            sendbuf[h][pl.ds(g2 * ny, ny)] = moved.reshape(ny, chunk, moved.shape[1])
            for dy in range(ny):
                d = g2 * ny + (y + dy) % ny

                @pl.when(d != me)
                def _():
                    point_copy(h, d, me).start()

            return 0

        lax.fori_loop(0, ng, body, 0)
        recvbuf[h][me] = sendbuf[h][me]

    for h in range(len(pieces)):
        dispatch(h)
        ring_step(h + 1)
    for step in range(len(pieces) + 1, 5):
        ring_step(step)

    others(slab, me, lambda s: target_copy(s, s).wait_recv())
    for q in range(max(1, slab // per)):
        tile = trecv[q * per]
        for s in range(q * per + 1, min(slab, (q + 1) * per)):
            tile = tile + trecv[s]
        tall[:, q * 128 : (q + 1) * 128] = tile

    def norms(j, _):
        block = table[j].astype(F32)
        column = jnp.sum(block * block, axis=1, keepdims=True)
        cnorm[j] = jnp.broadcast_to(column, (BS, 128)).T[:8]
        return 0

    lax.fori_loop(0, NZ, norms, 0)

    def rows_of(h, j):
        return recvbuf[h][:, pl.ds(pl.multiple_of(j * DEPTH, DEPTH), DEPTH), :].reshape(nrow, -1)

    def add_up(h):
        def body(j, _):
            want = tall[pl.ds(j, 1), :][:, :nrow]
            centroid = lax.broadcasted_iota(jnp.int32, (BS, nrow), 0).astype(F32) + 1.0
            hot = jnp.where(want == centroid, 1.0, 0.0).astype(BF16)
            sums[j, :, pieces[h]] = jnp.dot(hot, rows_of(h, j), preferred_element_type=F32)
            if h == 0:
                csend[j] = lax.dot_general(jnp.ones((8, nrow), BF16), hot, NT, preferred_element_type=F32)
            return 0

        lax.fori_loop(0, NZ, body, 0)

    def measure(h):
        def body(j, _):
            rows = rows_of(h, j)
            wide = rows.astype(F32)
            cross = lax.dot_general(
                rows, table[j, :, pieces[h]], NT, preferred_element_type=F32
            )
            part = jnp.sum(wide * wide, axis=1, keepdims=True) - 2.0 * cross
            if h > 0:
                part = part + partial[j]
            if h < len(pieces) - 1:
                partial[j] = part
            else:
                whole = (part + cnorm[j, :1, :]) / width
                dsend[:, pl.ds(pl.multiple_of(j * DEPTH, DEPTH), DEPTH), :] = whole.astype(BF16).reshape(
                    slab, DEPTH, BS
                )
            return 0

        lax.fori_loop(0, NZ, body, 0)

    half = BS // 2

    def reduce_copy(h, way, step):
        rows = pl.ds(way * half, half)
        src = rsend[h].at[way, step, rows] if step == 0 else rsend[h].at[way, step]
        dst = rrecv[h].at[way, step, rows] if step == 0 else rrecv[h].at[way, step]
        return remote(src, dst, r_send.at[h, way, step], r_recv.at[h, way, step], along(1 if way == 0 else -1))

    def reduce_step(h, step):
        piece = pieces[h]
        for way in range(2):
            lo, hi = way * half, (way + 1) * half
            if step == 0:
                rsend[h][way, 0, lo:hi] = sums[(z + 4) % NZ, lo:hi, piece].astype(BF16)
            else:
                target = (z + 4 - step) % NZ if way == 0 else (z + 4 + step) % NZ
                reduce_copy(h, way, step - 1).wait_recv()
                if step == 1:
                    olo, ohi = (1 - way) * half, (2 - way) * half
                    rsend[h][way, 1, lo:hi] = (
                        sums[target, lo:hi, piece] + rrecv[h][way, 0, lo:hi].astype(F32)
                    ).astype(BF16)
                    rsend[h][way, 1, olo:ohi] = sums[target, olo:ohi, piece].astype(BF16)
                else:
                    rsend[h][way, step] = (
                        sums[target, :, piece] + rrecv[h][way, step - 1].astype(F32)
                    ).astype(BF16)
            reduce_copy(h, way, step).start()

    def finish(h):
        piece = pieces[h]
        for way in range(2):
            reduce_copy(h, way, 3).wait_recv()
        if h == 0:
            others(NZ, z, lambda z2: count_copy(z2, z2).wait_recv())
            total = csend[z]
            crecv[z] = total
            total = crecv[0]
            for z2 in range(1, NZ):
                total = total + crecv[z2]
            denom[...] = jnp.broadcast_to(total[:1], (128, BS)).T + 1.0
        own = (
            sums[z, :, piece] + rrecv[h][0, 3].astype(F32) + rrecv[h][1, 3].astype(F32)
            + table[z, :, piece].astype(F32)
        )
        share = width // ng
        for q in range(own.shape[1] // share):
            g2 = piece.start // share + q
            fsend[g2] = (own[:, q * share : (q + 1) * share] / denom[:, :share]).astype(BF16)

            @pl.when(g2 != g)
            def _():
                fresh_copy(g2, g).start()

    def give_back(i, _):
        dx, dc = offset(i)
        g2 = ((x + dx) % nx) * nc + (c + dc) % nc
        for dy in range(ny):
            d = g2 * ny + (y + dy) % ny

            @pl.when(d != me)
            def _():
                dist_copy(d, me).start()

        return 0

    for h in range(len(pieces)):
        others(slab, me, lambda s: point_copy(h, s, s).wait_recv())
        add_up(h)
        if h == 0:
            others(NZ, z, lambda z2: count_copy(z2, z).start())
        reduce_step(h, 0)
        measure(h)
        if h == len(pieces) - 1:
            lax.fori_loop(0, ng, give_back, 0)
            dret[me] = dsend[me]
        for step in range(1, 4):
            reduce_step(h, step)
        finish(h)

    def bring(i, _):
        dx, dc = offset(i)
        g2 = ((x + nx - dx) % nx) * nc + (c + dc) % nc
        for dy in range(ny):
            d = g2 * ny + dy

            @pl.when(d != me)
            def _():
                dist_copy(d, d).wait_recv()

        hot = lax.broadcasted_iota(jnp.int32, (npoints, ny * chunk), 1) + g2 * (ny * chunk) == slots_col[:, :1]
        part = jnp.dot(
            jnp.where(hot, 1.0, 0.0).astype(BF16), dret[pl.ds(g2 * ny, ny)].reshape(ny * chunk, BS),
            preferred_element_type=F32,
        )

        @pl.when(i == 0)
        def _():
            acc[...] = part

        @pl.when(i > 0)
        def _():
            acc[...] += part

        return 0

    lax.fori_loop(0, ng, bring, 0)
    dist_out[...] = acc[...].astype(BF16)

    others(ng, g, lambda g2: fresh_copy(g2, g2).wait_recv())
    frecv[g] = fsend[g]

    others(slab, me, lambda d: target_copy(d, me).wait_send())
    others(slab, me, lambda d: dist_copy(d, me).wait_send())
    others(NZ, z, lambda z2: count_copy(z2, z).wait_send())
    others(ng, g, lambda g2: fresh_copy(g2, g).wait_send())
    for way in range(2):
        for step in range(4):
            ring_copy(way, step, 0).wait_send()
    for h in range(len(pieces)):
        others(slab, me, lambda d: point_copy(h, d, me).wait_send())
        for way in range(2):
            for step in range(4):
                reduce_copy(h, way, step).wait_send()


def bounds(width):
    edges = [0]
    for part in SPLIT:
        edges.append(edges[-1] + part * width // sum(SPLIT))
    return list(zip(edges[:-1], edges[1:]))


def fused(blocks, finals, points, centroids, dims):
    nx, nc, ny = dims
    ng, slab = nx * nc, nx * nc * ny
    npoints, width = points.shape
    chunk, share = NZ * DEPTH, width // (nx * nc)
    sizes = [b - a for a, b in bounds(width)]
    n = len(sizes)
    vmem, dma = pltpu.VMEM, pltpu.SemaphoreType.DMA
    tall_lanes = max(1, slab * DEPTH // 128) * 128
    return pl.pallas_call(
        functools.partial(kernel, dims),
        out_shape=(
            jax.ShapeDtypeStruct((npoints, BS), BF16),
            jax.ShapeDtypeStruct((ng, BS, share), BF16),
        ),
        in_specs=[pl.BlockSpec(memory_space=vmem)] * 3 + [pl.BlockSpec(memory_space=pl.ANY)],
        out_specs=(pl.BlockSpec(memory_space=vmem),) * 2,
        scratch_shapes=[
            tuple(vmem((slab, chunk, size), BF16) for size in sizes),
            tuple(vmem((slab, chunk, size), BF16) for size in sizes),
            tuple(vmem((2, 4, BS, size), BF16) for size in sizes),
            tuple(vmem((2, 4, BS, size), BF16) for size in sizes),
            vmem((NZ, BS, width), BF16),
            vmem((NZ, BS, width), F32),
            vmem((NZ, slab * DEPTH, BS), F32),
            vmem((slab, chunk, BS), BF16),
            vmem((slab, chunk, BS), BF16),
            vmem((slab, NZ, 128), F32),
            vmem((slab, NZ, 128), F32),
            vmem((NZ, tall_lanes), F32),
            vmem((NZ, 8, BS), F32),
            vmem((NZ, 8, BS), F32),
            vmem((NZ, 8, BS), F32),
            vmem((BS, 128), F32),
            vmem((ng, BS, share), BF16),
            vmem((npoints, BS), F32),
            vmem((1, npoints), jnp.int32),
            vmem((npoints, 128), jnp.int32),
            dma((n, slab)), dma((n, slab)), dma((slab,)), dma((slab,)), dma((slab,)), dma((slab,)),
            dma((2, 4)), dma((2, 4)), dma((n, 2, 4)), dma((n, 2, 4)),
            dma((NZ,)), dma((NZ,)), dma((ng,)), dma((ng,)), dma,
        ],
        compiler_params=pltpu.CompilerParams(
            collective_id=0, has_side_effects=True, vmem_limit_bytes=67043328
        ),
    )(blocks.reshape(1, npoints), finals[None, :], points, centroids)


def shards(points, blocks, finals, centroids):
    dims = tuple(lax.axis_size(a) for a in ("x", "core", "y"))
    distances, refreshed = fused(blocks, finals, points, centroids, dims)
    return distances, refreshed.reshape(-1, refreshed.shape[2]).astype(F32)


def solution(mesh):
    ngrp, ndev = mesh.shape["grp"], mesh.shape["dev"]
    fine = Mesh(mesh.devices.reshape(ngrp // 2, 2, NZ, ndev // NZ), ("x", "core", "z", "y"))
    rows = ("x", "core", "z", "y")
    return jax.shard_map(
        shards,
        mesh=fine,
        in_specs=(P(rows, None), P(rows, None), P(rows), P(("z", "y"), None)),
        out_specs=(P(rows, None), P(("z", "y"), ("x", "core"))),
        check_vma=False,
    )
```

```python
import functools

import jax
import jax.numpy as jnp
from jax import lax
from jax.experimental import pallas as pl
from jax.experimental.pallas import tpu as pltpu
from jax.sharding import Mesh, PartitionSpec as P

BS = 256
NZ = 8
SPLIT = (4, 2, 2)
ROOM = 112
DEPTH = 16
MESH = pl.DeviceIdType.MESH
F32, BF16 = jnp.float32, jnp.bfloat16
NT = (((1,), (1,)), ((), ()))


def kernel(
    dims, room, blocks_row, finals_row, points_in, centroids, dist_out, fresh_out, flag_out,
    points, sendbuf, recvbuf, opened, rsend, rrecv, table, sums, partial, dsend, dret, tsend, trecv, tall,
    csend, crecv, cnorm, denom, fsend, acc, slots_row, slots_col,
    p_send, p_recv, t_send, t_recv, d_send, d_recv, g_send, g_recv, r_send, r_recv,
    c_send, c_recv, f_send, f_recv, local_sem, points_sem,
):
    nx, nc, ny = dims
    ng = nx * nc
    slab = ng * ny
    x, c, z, y = (lax.axis_index(a) for a in ("x", "core", "z", "y"))
    g = x * nc + c
    me = g * ny + y
    npoints, width = points.shape
    pieces = [slice(a, b) for a, b in bounds(width)]
    frecv = fresh_out
    chunk = NZ * DEPTH
    nrow = slab * DEPTH
    per = 128 // DEPTH

    def at(d):
        g2 = d // ny
        return (g2 // nc, g2 % nc, z, d % ny)

    def along(step):
        return (x, c, (z + step + NZ) % NZ, y)

    def remote(src, dst, ssem, rsem, dev):
        return pltpu.make_async_remote_copy(
            src_ref=src, dst_ref=dst, send_sem=ssem, recv_sem=rsem, device_id=dev, device_id_type=MESH
        )

    def point_copy(h, d, slot):
        return remote(sendbuf[h].at[d], recvbuf[h].at[slot], p_send.at[h, d], p_recv.at[h, slot], at(d))

    def target_copy(d, slot):
        return remote(tsend.at[d], trecv.at[slot], t_send.at[d], t_recv.at[slot], at(d))

    def dist_copy(d, slot):
        return remote(dsend.at[d], dret.at[slot], d_send.at[d], d_recv.at[slot], at(d))

    def count_copy(z2, slot):
        return remote(csend.at[z2], crecv.at[slot], c_send.at[z2], c_recv.at[slot], (x, c, z2, y))

    def fresh_copy(g2, slot):
        return remote(fsend.at[g2], frecv.at[slot], f_send.at[g2], f_recv.at[slot], (g2 // nc, g2 % nc, z, y))

    def others(n, own, fn):
        def body(i, _):
            @pl.when(i != own)
            def _():
                fn(i)

            return 0

        lax.fori_loop(0, n, body, 0)

    def offset(i):
        turn = (2 * (i % nx) + 1) % 5 if nx == 4 else i % nx
        return turn, i // nx

    barrier = pltpu.get_barrier_semaphore()
    others(slab, me, lambda d: pl.semaphore_signal(barrier, inc=1, device_id=at(d), device_id_type=MESH))
    others(
        NZ, z, lambda z2: pl.semaphore_signal(barrier, inc=1, device_id=(x, c, z2, y), device_id_type=MESH)
    )
    own_copy = pltpu.make_async_copy(
        centroids.at[pl.ds(pl.multiple_of(g * BS, BS), BS)], table.at[z], local_sem
    )
    own_copy.start()
    points_copy = pltpu.make_async_copy(points_in, points, points_sem)
    points_copy.start()

    ids = blocks_row[...]
    dest = ((ids & (ng - 1)) * ny + (lax.shift_right_logical(ids, ng.bit_length() - 1) & (ny - 1))) * NZ
    dest = dest + lax.shift_right_logical(ids, (ng * ny).bit_length() - 1)
    strip = min(256, npoints)
    earlier = lax.broadcasted_iota(jnp.int32, (strip, strip), 0) < lax.broadcasted_iota(jnp.int32, (strip, strip), 1)
    earlier = jnp.where(earlier, 1.0, 0.0).astype(BF16)
    strips = [dest[:, q * strip : (q + 1) * strip] for q in range(npoints // strip)]
    members = [
        jnp.where(lax.broadcasted_iota(jnp.int32, (slab * NZ, strip), 0) == part, 1.0, 0.0) for part in strips
    ]
    held = [jnp.sum(member, axis=1, keepdims=True) for member in members]
    load = functools.reduce(lambda a, b: a + b, held)
    above = lax.broadcasted_iota(jnp.int32, (slab * NZ, slab * NZ), 0)
    left = lax.broadcasted_iota(jnp.int32, (slab * NZ, slab * NZ), 1)
    prior = jnp.where((left < above) & (left // NZ == above // NZ), 1.0, 0.0).astype(BF16)
    first = jnp.dot(
        prior, jnp.broadcast_to(load, (slab * NZ, 128)).astype(BF16), preferred_element_type=F32
    )[:, :1]
    seen = jnp.zeros((slab * NZ, 1), F32)
    ranks, firsts = [], []
    for member, more in zip(members, held):
        before = jnp.dot(member.astype(BF16), earlier, preferred_element_type=F32) + seen
        ranks.append(jnp.sum(member * before, axis=0, keepdims=True))
        firsts.append(jnp.sum(member * first, axis=0, keepdims=True))
        seen = seen + more
    rank = jnp.concatenate(ranks, axis=1).astype(jnp.int32)
    slots = dest * DEPTH + rank
    slots_col[...] = jnp.broadcast_to(slots.astype(F32), (128, npoints)).T.astype(jnp.int32)
    compact = room < chunk
    holder = lax.shift_right_logical(dest, NZ.bit_length() - 1)
    if compact:
        spot = rank + jnp.concatenate(firsts, axis=1).astype(jnp.int32)
        over = jnp.max(jnp.where(spot >= room, 1.0, 0.0), axis=1, keepdims=True)
        slots_row[...] = jnp.where(spot < room, holder * room + spot, -1)
    else:
        slots_row[...] = slots

    value = (finals_row[...] + 1).astype(F32)
    which = lax.broadcasted_iota(jnp.int32, (slab * NZ, npoints), 0) == dest
    place = lax.broadcasted_iota(jnp.int32, (128, npoints), 0) == rank + (me % per) * DEPTH
    tiles = lax.dot_general(
        jnp.where(which, value, 0.0).astype(BF16), jnp.where(place, 1.0, 0.0).astype(BF16), NT,
        preferred_element_type=F32,
    )
    tsend[:, :NZ, :] = tiles.reshape(slab, NZ, 128)
    if compact:
        origin = (slots - holder * chunk + 1).astype(F32)
        to = lax.broadcasted_iota(jnp.int32, (slab, npoints), 0) == holder
        row = lax.broadcasted_iota(jnp.int32, (128, npoints), 0) == spot
        origins = lax.dot_general(
            jnp.where(to, origin, 0.0).astype(BF16), jnp.where(row, 1.0, 0.0).astype(BF16), NT,
            preferred_element_type=F32,
        )
        line = lax.broadcasted_iota(jnp.int32, (slab, NZ, 128), 1)
        tsend[:, NZ:, :] = jnp.where(line == 0, origins[:, None, :], over[None])
    trecv[me] = tsend[me]
    own_copy.wait()
    pl.semaphore_wait(barrier, slab - 1 + NZ - 1)
    others(slab, me, lambda d: target_copy(d, me).start())

    def ring_copy(way, step, back):
        step_z = 1 if way == 0 else -1
        owner = (z - step_z * (step - back) + 2 * NZ) % NZ if not back else (z - step_z * (step + 1) + 2 * NZ) % NZ
        rows = slice(None) if step < 3 else pl.ds(way * (BS // 2), BS // 2)
        ref = table.at[owner, rows] if step == 3 else table.at[owner]
        return remote(ref, ref, g_send.at[way, step], g_recv.at[way, step], along(step_z))

    def ring_step(step):
        for way in range(2):
            if step:
                ring_copy(way, step - 1, 1).wait_recv()
            if step < 4:
                ring_copy(way, step, 0).start()

    ring_step(0)
    points_copy.wait()

    def dispatch(h):
        def body(i, _):
            dx, dc = offset(i)
            g2 = ((x + dx) % nx) * nc + (c + dc) % nc
            hot = lax.broadcasted_iota(jnp.int32, (ny * room, npoints), 0) + g2 * (ny * room) == slots_row[...]
            moved = jnp.dot(
                jnp.where(hot, 1.0, 0.0).astype(BF16), points[:, pieces[h]],
                preferred_element_type=F32,
            ).astype(BF16)
            sendbuf[h][pl.ds(g2 * ny, ny)] = moved.reshape(ny, room, moved.shape[1])
            for dy in range(ny):
                d = g2 * ny + (y + dy) % ny

                @pl.when(d != me)
                def _():
                    point_copy(h, d, me).start()

            return 0

        lax.fori_loop(0, ng, body, 0)
        recvbuf[h][me] = sendbuf[h][me]

    for h in range(len(pieces)):
        dispatch(h)
        ring_step(h + 1)
    for step in range(len(pieces) + 1, 5):
        ring_step(step)

    others(slab, me, lambda s: target_copy(s, s).wait_recv())
    for q in range(max(1, slab // per)):
        tile = trecv[q * per]
        for s in range(q * per + 1, min(slab, (q + 1) * per)):
            tile = tile + trecv[s]
        tall[:, q * 128 : (q + 1) * 128] = tile

    def norms(j, _):
        block = table[j].astype(F32)
        column = jnp.sum(block * block, axis=1, keepdims=True)
        cnorm[j] = jnp.broadcast_to(column, (BS, 128)).T[:8]
        return 0

    lax.fori_loop(0, NZ, norms, 0)

    def expand(h):
        size = pieces[h].stop - pieces[h].start

        def body(i, _):
            for k in range(4):
                s = i * 4 + k
                slot = lax.broadcasted_iota(jnp.int32, (chunk, room), 0).astype(F32) + 1.0
                hot = jnp.where(trecv[s, NZ : NZ + 1, :room] == slot, 1.0, 0.0).astype(BF16)
                opened[s, :, :size] = jnp.dot(hot, recvbuf[h][s], preferred_element_type=F32).astype(BF16)
            return 0

        if compact:
            lax.fori_loop(0, slab // 4, body, 0)

    def rows_of(h, j):
        size = pieces[h].stop - pieces[h].start
        if compact:
            return opened[:, pl.ds(pl.multiple_of(j * DEPTH, DEPTH), DEPTH), :size].reshape(nrow, size)
        return recvbuf[h][:, pl.ds(pl.multiple_of(j * DEPTH, DEPTH), DEPTH), :].reshape(nrow, -1)

    def add_up(h):
        def body(j, _):
            want = tall[pl.ds(j, 1), :nrow]
            centroid = lax.broadcasted_iota(jnp.int32, (BS, nrow), 0).astype(F32) + 1.0
            hot = jnp.where(want == centroid, 1.0, 0.0).astype(BF16)
            sums[j, :, pieces[h]] = jnp.dot(hot, rows_of(h, j), preferred_element_type=F32)
            if h == 0:
                number = lax.dot_general(jnp.ones((8, nrow), BF16), hot, NT, preferred_element_type=F32)
                if compact:
                    line = lax.broadcasted_iota(jnp.int32, (8, BS), 0)
                    short = jnp.sum(tall[NZ + 1 : NZ + 2, :], axis=1, keepdims=True)
                    number = jnp.where(line == 0, number, short)
                csend[j] = number
            return 0

        lax.fori_loop(0, NZ, body, 0)

    def measure(h):
        def body(j, _):
            rows = rows_of(h, j)
            wide = rows.astype(F32)
            cross = lax.dot_general(
                rows, table[j, :, pieces[h]], NT, preferred_element_type=F32
            )
            part = jnp.sum(wide * wide, axis=1, keepdims=True) - 2.0 * cross
            if h > 0:
                part = part + partial[j]
            if h < len(pieces) - 1:
                partial[j] = part
            else:
                whole = (part + cnorm[j, :1, :]) / width
                dsend[:, pl.ds(pl.multiple_of(j * DEPTH, DEPTH), DEPTH), :] = whole.astype(BF16).reshape(
                    slab, DEPTH, BS
                )
            return 0

        lax.fori_loop(0, NZ, body, 0)

    half = BS // 2

    def reduce_copy(h, way, step):
        rows = pl.ds(way * half, half)
        src = rsend[h].at[way, step, rows] if step == 0 else rsend[h].at[way, step]
        dst = rrecv[h].at[way, step, rows] if step == 0 else rrecv[h].at[way, step]
        return remote(src, dst, r_send.at[h, way, step], r_recv.at[h, way, step], along(1 if way == 0 else -1))

    def reduce_step(h, step):
        piece = pieces[h]
        for way in range(2):
            lo, hi = way * half, (way + 1) * half
            if step == 0:
                rsend[h][way, 0, lo:hi] = sums[(z + 4) % NZ, lo:hi, piece].astype(BF16)
            else:
                target = (z + 4 - step) % NZ if way == 0 else (z + 4 + step) % NZ
                reduce_copy(h, way, step - 1).wait_recv()
                if step == 1:
                    olo, ohi = (1 - way) * half, (2 - way) * half
                    rsend[h][way, 1, lo:hi] = (
                        sums[target, lo:hi, piece] + rrecv[h][way, 0, lo:hi].astype(F32)
                    ).astype(BF16)
                    rsend[h][way, 1, olo:ohi] = sums[target, olo:ohi, piece].astype(BF16)
                else:
                    rsend[h][way, step] = (
                        sums[target, :, piece] + rrecv[h][way, step - 1].astype(F32)
                    ).astype(BF16)
            reduce_copy(h, way, step).start()

    def finish(h):
        piece = pieces[h]
        for way in range(2):
            reduce_copy(h, way, 3).wait_recv()
        if h == 0:
            others(NZ, z, lambda z2: count_copy(z2, z2).wait_recv())
            total = csend[z]
            crecv[z] = total
            total = crecv[0]
            for z2 in range(1, NZ):
                total = total + crecv[z2]
            flag_out[...] = jnp.broadcast_to(total[1:2, :128], (8, 128))
            denom[...] = jnp.broadcast_to(total[:1], (128, BS)).T + 1.0
        own = (
            sums[z, :, piece] + rrecv[h][0, 3].astype(F32) + rrecv[h][1, 3].astype(F32)
            + table[z, :, piece].astype(F32)
        )
        share = width // ng
        for q in range(own.shape[1] // share):
            g2 = piece.start // share + q
            fsend[g2] = (own[:, q * share : (q + 1) * share] / denom[:, :share]).astype(BF16)

            @pl.when(g2 != g)
            def _():
                fresh_copy(g2, g).start()

    def give_back(i, _):
        dx, dc = offset(i)
        g2 = ((x + dx) % nx) * nc + (c + dc) % nc
        for dy in range(ny):
            d = g2 * ny + (y + dy) % ny

            @pl.when(d != me)
            def _():
                dist_copy(d, me).start()

        return 0

    def arrived(h):
        others(slab, me, lambda s: point_copy(h, s, s).wait_recv())

    last = len(pieces) - 1
    for h in range(last):
        arrived(h)
        expand(h)
        add_up(h)
        if h == 0:
            others(NZ, z, lambda z2: count_copy(z2, z).start())
        reduce_step(h, 0)
        measure(h)
        for step in range(1, 4 if h < last - 1 else 3):
            reduce_step(h, step)
        if h < last - 1:
            finish(h)
    arrived(last)
    expand(last)
    measure(last)
    lax.fori_loop(0, ng, give_back, 0)
    dret[me] = dsend[me]
    add_up(last)
    reduce_step(last, 0)
    reduce_step(last - 1, 3)
    finish(last - 1)
    for step in range(1, 4):
        reduce_step(last, step)
    finish(last)

    def bring(i, _):
        dx, dc = offset(i)
        g2 = ((x + nx - dx) % nx) * nc + (c + dc) % nc
        for dy in range(ny):
            d = g2 * ny + dy

            @pl.when(d != me)
            def _():
                dist_copy(d, d).wait_recv()

        hot = lax.broadcasted_iota(jnp.int32, (npoints, ny * chunk), 1) + g2 * (ny * chunk) == slots_col[:, :1]
        part = jnp.dot(
            jnp.where(hot, 1.0, 0.0).astype(BF16), dret[pl.ds(g2 * ny, ny)].reshape(ny * chunk, BS),
            preferred_element_type=F32,
        )

        @pl.when(i == 0)
        def _():
            acc[...] = part

        @pl.when(i > 0)
        def _():
            acc[...] += part

        return 0

    lax.fori_loop(0, ng, bring, 0)
    dist_out[...] = acc[...].astype(BF16)

    others(ng, g, lambda g2: fresh_copy(g2, g2).wait_recv())
    frecv[g] = fsend[g]

    others(slab, me, lambda d: target_copy(d, me).wait_send())
    others(slab, me, lambda d: dist_copy(d, me).wait_send())
    others(NZ, z, lambda z2: count_copy(z2, z).wait_send())
    others(ng, g, lambda g2: fresh_copy(g2, g).wait_send())
    for way in range(2):
        for step in range(4):
            ring_copy(way, step, 0).wait_send()
    for h in range(len(pieces)):
        others(slab, me, lambda d: point_copy(h, d, me).wait_send())
        for way in range(2):
            for step in range(4):
                reduce_copy(h, way, step).wait_send()


def bounds(width):
    edges = [0]
    for part in SPLIT:
        edges.append(edges[-1] + part * width // sum(SPLIT))
    return list(zip(edges[:-1], edges[1:]))


def fused(blocks, finals, points, centroids, dims, room, name):
    nx, nc, ny = dims
    ng, slab = nx * nc, nx * nc * ny
    npoints, width = points.shape
    chunk, share = NZ * DEPTH, width // (nx * nc)
    sizes = [b - a for a, b in bounds(width)]
    n = len(sizes)
    vmem, dma = pltpu.VMEM, pltpu.SemaphoreType.DMA
    lines = 2 * NZ if room < chunk else NZ
    tall_lanes = max(1, slab * DEPTH // 128) * 128
    return pl.pallas_call(
        functools.partial(kernel, dims, room),
        out_shape=(
            jax.ShapeDtypeStruct((npoints, BS), BF16),
            jax.ShapeDtypeStruct((ng, BS, share), BF16),
            jax.ShapeDtypeStruct((8, 128), F32),
        ),
        in_specs=[pl.BlockSpec(memory_space=vmem)] * 2 + [pl.BlockSpec(memory_space=pl.ANY)] * 2,
        out_specs=(pl.BlockSpec(memory_space=vmem),) * 3,
        scratch_shapes=[
            vmem((npoints, width), BF16),
            tuple(vmem((slab, room, size), BF16) for size in sizes),
            tuple(vmem((slab, room, size), BF16) for size in sizes),
            vmem((slab, chunk, max(sizes)) if room < chunk else (8, 128), BF16),
            tuple(vmem((2, 4, BS, size), BF16) for size in sizes),
            tuple(vmem((2, 4, BS, size), BF16) for size in sizes),
            vmem((NZ, BS, width), BF16),
            vmem((NZ, BS, width), F32),
            vmem((NZ, slab * DEPTH, BS), F32),
            vmem((slab, chunk, BS), BF16),
            vmem((slab, chunk, BS), BF16),
            vmem((slab, lines, 128), F32),
            vmem((slab, lines, 128), F32),
            vmem((lines, tall_lanes), F32),
            vmem((NZ, 8, BS), F32),
            vmem((NZ, 8, BS), F32),
            vmem((NZ, 8, BS), F32),
            vmem((BS, 128), F32),
            vmem((ng, BS, share), BF16),
            vmem((npoints, BS), F32),
            vmem((1, npoints), jnp.int32),
            vmem((npoints, 128), jnp.int32),
            dma((n, slab)), dma((n, slab)), dma((slab,)), dma((slab,)), dma((slab,)), dma((slab,)),
            dma((2, 4)), dma((2, 4)), dma((n, 2, 4)), dma((n, 2, 4)),
            dma((NZ,)), dma((NZ,)), dma((ng,)), dma((ng,)), dma, dma,
        ],
        compiler_params=pltpu.CompilerParams(
            collective_id=name, has_side_effects=True, vmem_limit_bytes=67043328
        ),
    )(blocks.reshape(1, npoints), finals[None, :], points, centroids)


def shards(points, blocks, finals, centroids):
    dims = tuple(lax.axis_size(a) for a in ("x", "core", "y"))
    distances, refreshed, flag = fused(blocks, finals, points, centroids, dims, ROOM, 0)
    if ROOM < NZ * DEPTH:
        distances, refreshed = lax.cond(
            flag[0, 0] > 0.5,
            lambda: fused(blocks, finals, points, centroids, dims, NZ * DEPTH, 1)[:2],
            lambda: (distances, refreshed),
        )
    return distances, refreshed.reshape(-1, refreshed.shape[2]).astype(F32)


def solution(mesh):
    ngrp, ndev = mesh.shape["grp"], mesh.shape["dev"]
    fine = Mesh(mesh.devices.reshape(ngrp // 2, 2, NZ, ndev // NZ), ("x", "core", "z", "y"))
    rows = ("x", "core", "z", "y")
    return jax.shard_map(
        shards,
        mesh=fine,
        in_specs=(P(rows, None), P(rows, None), P(rows), P(("z", "y"), None)),
        out_specs=(P(rows, None), P(("z", "y"), ("x", "core"))),
        check_vma=False,
    )
```

```python
import functools

import jax
import jax.numpy as jnp
from jax import lax
from jax.experimental import pallas as pl
from jax.experimental.pallas import tpu as pltpu
from jax.sharding import Mesh, PartitionSpec as P

BS = 256
NZ = 8
SPLIT = (4, 2, 2)
DEPTH = 16
MESH = pl.DeviceIdType.MESH
F32, BF16 = jnp.float32, jnp.bfloat16
NT = (((1,), (1,)), ((), ()))


def kernel(
    dims, blocks_row, finals_row, points_in, centroids, dist_out, fresh_out,
    points, sendbuf, recvbuf, rsend, rrecv, table, sums, partial, dsend, dret, tsend, trecv, tall,
    csend, crecv, cnorm, denom, fsend, acc, near, slots_row, slots_col,
    p_send, p_recv, t_send, t_recv, d_send, d_recv, g_send, g_recv, r_send, r_recv,
    c_send, c_recv, f_send, f_recv, local_sem, points_sem,
):
    nx, nc, ny = dims
    ng = nx * nc
    slab = ng * ny
    x, c, z, y = (lax.axis_index(a) for a in ("x", "core", "z", "y"))
    g = x * nc + c
    me = g * ny + y
    npoints, width = points.shape
    pieces = [slice(a, b) for a, b in bounds(width)]
    frecv = fresh_out
    chunk = NZ * DEPTH
    nrow = slab * DEPTH
    per = 128 // DEPTH

    def at(d):
        g2 = d // ny
        return (g2 // nc, g2 % nc, z, d % ny)

    def along(step):
        return (x, c, (z + step + NZ) % NZ, y)

    def remote(src, dst, ssem, rsem, dev):
        return pltpu.make_async_remote_copy(
            src_ref=src, dst_ref=dst, send_sem=ssem, recv_sem=rsem, device_id=dev, device_id_type=MESH
        )

    def point_copy(h, d, slot):
        return remote(sendbuf[h].at[d], recvbuf[h].at[slot], p_send.at[h, d], p_recv.at[h, slot], at(d))

    def target_copy(d, slot):
        return remote(tsend.at[d], trecv.at[slot], t_send.at[d], t_recv.at[slot], at(d))

    def dist_copy(d, slot):
        return remote(dsend.at[d], dret.at[slot], d_send.at[d], d_recv.at[slot], at(d))

    def count_copy(z2, slot):
        return remote(csend.at[z2], crecv.at[slot], c_send.at[z2], c_recv.at[slot], (x, c, z2, y))

    def fresh_copy(g2, slot):
        return remote(fsend.at[g2], frecv.at[slot], f_send.at[g2], f_recv.at[slot], (g2 // nc, g2 % nc, z, y))

    def others(n, own, fn):
        def body(i, _):
            @pl.when(i != own)
            def _():
                fn(i)

            return 0

        lax.fori_loop(0, n, body, 0)

    def offset(i):
        turn = (2 * (i % nx) + 1) % 5 if nx == 4 else i % nx
        return turn, i // nx

    barrier = pltpu.get_barrier_semaphore()
    others(slab, me, lambda d: pl.semaphore_signal(barrier, inc=1, device_id=at(d), device_id_type=MESH))
    others(
        NZ, z, lambda z2: pl.semaphore_signal(barrier, inc=1, device_id=(x, c, z2, y), device_id_type=MESH)
    )
    own_copy = pltpu.make_async_copy(
        centroids.at[pl.ds(pl.multiple_of(g * BS, BS), BS)], table.at[z], local_sem
    )
    own_copy.start()
    points_copy = pltpu.make_async_copy(points_in, points, points_sem)
    points_copy.start()

    ids = blocks_row[...]
    dest = ((ids & (ng - 1)) * ny + (lax.shift_right_logical(ids, ng.bit_length() - 1) & (ny - 1))) * NZ
    dest = dest + lax.shift_right_logical(ids, (ng * ny).bit_length() - 1)
    strip = min(256, npoints)
    earlier = lax.broadcasted_iota(jnp.int32, (strip, strip), 0) < lax.broadcasted_iota(jnp.int32, (strip, strip), 1)
    earlier = jnp.where(earlier, 1.0, 0.0).astype(BF16)
    strips = [dest[:, q * strip : (q + 1) * strip] for q in range(npoints // strip)]
    members = [
        jnp.where(lax.broadcasted_iota(jnp.int32, (slab * NZ, strip), 0) == part, 1.0, 0.0) for part in strips
    ]
    seen = jnp.zeros((slab * NZ, 1), F32)
    ranks = []
    for member in members:
        before = jnp.dot(member.astype(BF16), earlier, preferred_element_type=F32) + seen
        ranks.append(jnp.sum(member * before, axis=0, keepdims=True))
        seen = seen + jnp.sum(member, axis=1, keepdims=True)
    rank = jnp.concatenate(ranks, axis=1).astype(jnp.int32)
    slots = dest * DEPTH + rank
    slots_row[...] = slots
    slots_col[...] = jnp.broadcast_to(slots.astype(F32), (128, npoints)).T.astype(jnp.int32)

    value = (finals_row[...] + 1).astype(F32)
    which = lax.broadcasted_iota(jnp.int32, (slab * NZ, npoints), 0) == dest
    place = lax.broadcasted_iota(jnp.int32, (128, npoints), 0) == rank + (me % per) * DEPTH
    tiles = lax.dot_general(
        jnp.where(which, value, 0.0).astype(BF16), jnp.where(place, 1.0, 0.0).astype(BF16), NT,
        preferred_element_type=F32,
    )
    tsend[...] = tiles.reshape(slab, NZ, 128)
    trecv[me] = tsend[me]
    own_copy.wait()
    pl.semaphore_wait(barrier, slab - 1 + NZ - 1)
    others(slab, me, lambda d: target_copy(d, me).start())

    def ring_copy(way, step, back):
        step_z = 1 if way == 0 else -1
        owner = (z - step_z * (step - back) + 2 * NZ) % NZ if not back else (z - step_z * (step + 1) + 2 * NZ) % NZ
        rows = slice(None) if step < 3 else pl.ds(way * (BS // 2), BS // 2)
        ref = table.at[owner, rows] if step == 3 else table.at[owner]
        return remote(ref, ref, g_send.at[way, step], g_recv.at[way, step], along(step_z))

    def ring_step(step):
        for way in range(2):
            if step:
                ring_copy(way, step - 1, 1).wait_recv()
            if step < 4:
                ring_copy(way, step, 0).start()

    ring_step(0)
    points_copy.wait()

    def dispatch(h):
        def body(i, _):
            dx, dc = offset(i)
            g2 = ((x + dx) % nx) * nc + (c + dc) % nc
            hot = lax.broadcasted_iota(jnp.int32, (ny * chunk, npoints), 0) + g2 * (ny * chunk) == slots_row[...]
            moved = jnp.dot(
                jnp.where(hot, 1.0, 0.0).astype(BF16), points[:, pieces[h]],
                preferred_element_type=F32,
            ).astype(BF16)
            sendbuf[h][pl.ds(g2 * ny, ny)] = moved.reshape(ny, chunk, moved.shape[1])
            for dy in range(ny):
                d = g2 * ny + (y + dy) % ny

                @pl.when(d != me)
                def _():
                    point_copy(h, d, me).start()

            return 0

        lax.fori_loop(0, ng, body, 0)
        recvbuf[h][me] = sendbuf[h][me]

    for h in range(len(pieces)):
        dispatch(h)
        ring_step(h + 1)
    for step in range(len(pieces) + 1, 5):
        ring_step(step)

    others(slab, me, lambda s: target_copy(s, s).wait_recv())
    for q in range(max(1, slab // per)):
        tile = trecv[q * per]
        for s in range(q * per + 1, min(slab, (q + 1) * per)):
            tile = tile + trecv[s]
        tall[:, q * 128 : (q + 1) * 128] = tile

    def norms(j, _):
        block = table[j].astype(F32)
        column = jnp.sum(block * block, axis=1, keepdims=True)
        cnorm[j] = jnp.broadcast_to(column, (BS, 128)).T[:8]
        return 0

    lax.fori_loop(0, NZ, norms, 0)

    def rows_of(h, j):
        return recvbuf[h][:, pl.ds(pl.multiple_of(j * DEPTH, DEPTH), DEPTH), :].reshape(nrow, -1)

    def add_up(h):
        def body(j, _):
            want = tall[pl.ds(j, 1), :nrow]
            centroid = lax.broadcasted_iota(jnp.int32, (BS, nrow), 0).astype(F32) + 1.0
            hot = jnp.where(want == centroid, 1.0, 0.0).astype(BF16)
            sums[j, :, pieces[h]] = jnp.dot(hot, rows_of(h, j), preferred_element_type=F32)
            if h == 0:
                csend[j] = lax.dot_general(jnp.ones((8, nrow), BF16), hot, NT, preferred_element_type=F32)
            return 0

        lax.fori_loop(0, NZ, body, 0)

    def measure(h):
        def body(j, _):
            rows = rows_of(h, j)
            wide = rows.astype(F32)
            cross = lax.dot_general(
                rows, table[j, :, pieces[h]], NT, preferred_element_type=F32
            )
            part = jnp.sum(wide * wide, axis=1, keepdims=True) - 2.0 * cross
            if h > 0:
                part = part + partial[j]
            if h < len(pieces) - 1:
                partial[j] = part
            else:
                whole = (part + cnorm[j, :1, :]) / width
                dsend[:, pl.ds(pl.multiple_of(j * DEPTH, DEPTH), DEPTH), :] = whole.astype(BF16).reshape(
                    slab, DEPTH, BS
                )
            return 0

        lax.fori_loop(0, NZ, body, 0)

    half = BS // 2

    def reduce_copy(h, way, step):
        rows = pl.ds(way * half, half)
        src = rsend[h].at[way, step, rows] if step == 0 else rsend[h].at[way, step]
        dst = rrecv[h].at[way, step, rows] if step == 0 else rrecv[h].at[way, step]
        return remote(src, dst, r_send.at[h, way, step], r_recv.at[h, way, step], along(1 if way == 0 else -1))

    def reduce_step(h, step):
        piece = pieces[h]
        for way in range(2):
            lo, hi = way * half, (way + 1) * half
            if step == 0:
                rsend[h][way, 0, lo:hi] = sums[(z + 4) % NZ, lo:hi, piece].astype(BF16)
            else:
                target = (z + 4 - step) % NZ if way == 0 else (z + 4 + step) % NZ
                reduce_copy(h, way, step - 1).wait_recv()
                if step == 1:
                    olo, ohi = (1 - way) * half, (2 - way) * half
                    rsend[h][way, 1, lo:hi] = (
                        sums[target, lo:hi, piece] + rrecv[h][way, 0, lo:hi].astype(F32)
                    ).astype(BF16)
                    rsend[h][way, 1, olo:ohi] = sums[target, olo:ohi, piece].astype(BF16)
                else:
                    rsend[h][way, step] = (
                        sums[target, :, piece] + rrecv[h][way, step - 1].astype(F32)
                    ).astype(BF16)
            reduce_copy(h, way, step).start()

    def finish(h):
        piece = pieces[h]
        for way in range(2):
            reduce_copy(h, way, 3).wait_recv()
        if h == 0:
            others(NZ, z, lambda z2: count_copy(z2, z2).wait_recv())
            total = csend[z]
            crecv[z] = total
            total = crecv[0]
            for z2 in range(1, NZ):
                total = total + crecv[z2]
            denom[...] = jnp.broadcast_to(total[:1], (128, BS)).T + 1.0
        own = (
            sums[z, :, piece] + rrecv[h][0, 3].astype(F32) + rrecv[h][1, 3].astype(F32)
            + table[z, :, piece].astype(F32)
        )
        share = width // ng
        for q in range(own.shape[1] // share):
            g2 = piece.start // share + q
            fsend[g2] = (own[:, q * share : (q + 1) * share] / denom[:, :share]).astype(BF16)

            @pl.when(g2 != g)
            def _():
                fresh_copy(g2, g).start()

    def give_back(i, _):
        dx, dc = offset(i)
        g2 = ((x + dx) % nx) * nc + (c + dc) % nc
        for dy in range(ny):
            d = g2 * ny + (y + dy) % ny

            @pl.when(d != me)
            def _():
                dist_copy(d, me).start()

        return 0

    def arrived(h):
        others(slab, me, lambda s: point_copy(h, s, s).wait_recv())

    last = len(pieces) - 1
    for h in range(last):
        arrived(h)
        add_up(h)
        if h == 0:
            others(NZ, z, lambda z2: count_copy(z2, z).start())
        reduce_step(h, 0)
        measure(h)
        for step in range(1, 4 if h < last - 1 else 3):
            reduce_step(h, step)
        if h < last - 1:
            finish(h)
    arrived(last)
    measure(last)
    lax.fori_loop(0, ng, give_back, 0)
    dret[me] = dsend[me]
    add_up(last)
    reduce_step(last, 0)
    reduce_step(last - 1, 3)

    def bring(i):
        dx, dc = offset(i)
        g2 = ((x + nx - dx) % nx) * nc + (c + dc) % nc
        for dy in range(ny):
            d = g2 * ny + dy

            @pl.when(d != me)
            def _():
                dist_copy(d, d).wait_recv()

        hot = lax.broadcasted_iota(jnp.int32, (npoints, ny * chunk), 1) + g2 * (ny * chunk) == slots_col[:, :1]
        part = jnp.dot(
            jnp.where(hot, 1.0, 0.0).astype(BF16), dret[pl.ds(g2 * ny, ny)].reshape(ny * chunk, BS),
            preferred_element_type=F32,
        )

        @pl.when(i == 0)
        def _():
            acc[...] = part

        @pl.when(i > 0)
        def _():
            acc[...] += part

    def bring_some(low, high):
        def body(i, _):
            bring(i)
            return 0

        lax.fori_loop(low, high, body, 0)

    def sent(h):
        others(slab, me, lambda d: point_copy(h, d, me).wait_send())

    sent(0)
    reduce_step(last, 1)
    finish(last - 1)
    bring_some(0, ng // 4)
    for h in range(1, len(pieces)):
        sent(h)
    reduce_step(last, 2)
    others(slab, me, lambda d: target_copy(d, me).wait_send())
    others(NZ, z, lambda z2: count_copy(z2, z).wait_send())
    for way in range(2):
        for step in range(4):
            ring_copy(way, step, 0).wait_send()
    bring_some(ng // 4, ng // 2)
    reduce_step(last, 3)
    bring_some(ng // 2, 3 * ng // 4)
    finish(last)
    for h in range(len(pieces)):
        for way in range(2):
            for step in range(4):
                reduce_copy(h, way, step).wait_send()
    bring_some(3 * ng // 4, ng)
    near[...] = acc[...].astype(BF16)
    out_copy = pltpu.make_async_copy(near, dist_out, points_sem)
    out_copy.start()

    others(ng, g, lambda g2: fresh_copy(g2, g2).wait_recv())
    frecv[g] = fsend[g]
    others(slab, me, lambda d: dist_copy(d, me).wait_send())
    others(ng, g, lambda g2: fresh_copy(g2, g).wait_send())
    out_copy.wait()


def bounds(width):
    edges = [0]
    for part in SPLIT:
        edges.append(edges[-1] + part * width // sum(SPLIT))
    return list(zip(edges[:-1], edges[1:]))


def fused(blocks, finals, points, centroids, dims):
    nx, nc, ny = dims
    ng, slab = nx * nc, nx * nc * ny
    npoints, width = points.shape
    chunk, share = NZ * DEPTH, width // (nx * nc)
    sizes = [b - a for a, b in bounds(width)]
    n = len(sizes)
    vmem, dma = pltpu.VMEM, pltpu.SemaphoreType.DMA
    tall_lanes = max(1, slab * DEPTH // 128) * 128
    return pl.pallas_call(
        functools.partial(kernel, dims),
        out_shape=(
            jax.ShapeDtypeStruct((npoints, BS), BF16),
            jax.ShapeDtypeStruct((ng, BS, share), BF16),
        ),
        in_specs=[pl.BlockSpec(memory_space=vmem)] * 2 + [pl.BlockSpec(memory_space=pl.ANY)] * 2,
        out_specs=(pl.BlockSpec(memory_space=pl.ANY), pl.BlockSpec(memory_space=vmem)),
        scratch_shapes=[
            vmem((npoints, width), BF16),
            tuple(vmem((slab, chunk, size), BF16) for size in sizes),
            tuple(vmem((slab, chunk, size), BF16) for size in sizes),
            tuple(vmem((2, 4, BS, size), BF16) for size in sizes),
            tuple(vmem((2, 4, BS, size), BF16) for size in sizes),
            vmem((NZ, BS, width), BF16),
            vmem((NZ, BS, width), F32),
            vmem((NZ, slab * DEPTH, BS), F32),
            vmem((slab, chunk, BS), BF16),
            vmem((slab, chunk, BS), BF16),
            vmem((slab, NZ, 128), F32),
            vmem((slab, NZ, 128), F32),
            vmem((NZ, tall_lanes), F32),
            vmem((NZ, 8, BS), F32),
            vmem((NZ, 8, BS), F32),
            vmem((NZ, 8, BS), F32),
            vmem((BS, 128), F32),
            vmem((ng, BS, share), BF16),
            vmem((npoints, BS), F32),
            vmem((npoints, BS), BF16),
            vmem((1, npoints), jnp.int32),
            vmem((npoints, 128), jnp.int32),
            dma((n, slab)), dma((n, slab)), dma((slab,)), dma((slab,)), dma((slab,)), dma((slab,)),
            dma((2, 4)), dma((2, 4)), dma((n, 2, 4)), dma((n, 2, 4)),
            dma((NZ,)), dma((NZ,)), dma((ng,)), dma((ng,)), dma, dma,
        ],
        compiler_params=pltpu.CompilerParams(
            collective_id=0, has_side_effects=True, vmem_limit_bytes=67043328
        ),
    )(blocks.reshape(1, npoints), finals[None, :], points, centroids)


def shards(points, blocks, finals, centroids):
    dims = tuple(lax.axis_size(a) for a in ("x", "core", "y"))
    distances, refreshed = fused(blocks, finals, points, centroids, dims)
    return distances, refreshed.reshape(-1, refreshed.shape[2]).astype(F32)


def solution(mesh):
    ngrp, ndev = mesh.shape["grp"], mesh.shape["dev"]
    fine = Mesh(mesh.devices.reshape(ngrp // 2, 2, NZ, ndev // NZ), ("x", "core", "z", "y"))
    rows = ("x", "core", "z", "y")
    return jax.shard_map(
        shards,
        mesh=fine,
        in_specs=(P(rows, None), P(rows, None), P(rows), P(("z", "y"), None)),
        out_specs=(P(rows, None), P(("z", "y"), ("x", "core"))),
        check_vma=False,
    )
```

```python
import functools

import jax
import jax.numpy as jnp
from jax import lax
from jax.experimental import pallas as pl
from jax.experimental.pallas import tpu as pltpu
from jax.sharding import Mesh, PartitionSpec as P

BS = 256
NZ = 8
SPLIT = (4, 2, 2)
DEPTH = 16
MESH = pl.DeviceIdType.MESH
F32, BF16 = jnp.float32, jnp.bfloat16
NT = (((1,), (1,)), ((), ()))


def kernel(
    dims, blocks_row, finals_row, points_in, centroids, dist_out, fresh_out,
    points, sendbuf, recvbuf, rsend, rrecv, table, sums, partial, dsend, dret, tsend, trecv, tall,
    csend, crecv, cnorm, denom, fsend, acc, near, slots_row, slots_col,
    p_send, p_recv, t_send, t_recv, d_send, d_recv, g_send, g_recv, r_send, r_recv,
    c_send, c_recv, f_send, f_recv, local_sem, points_sem,
):
    nx, nc, ny = dims
    ng = nx * nc
    slab = ng * ny
    x, c, z, y = (lax.axis_index(a) for a in ("x", "core", "z", "y"))
    g = x * nc + c
    me = g * ny + y
    npoints, width = points.shape
    pieces = [slice(a, b) for a, b in bounds(width)]
    frecv = fresh_out
    chunk = NZ * DEPTH
    nrow = slab * DEPTH
    per = 128 // DEPTH

    def at(d):
        g2 = d // ny
        return (g2 // nc, g2 % nc, z, d % ny)

    def along(step):
        return (x, c, (z + step + NZ) % NZ, y)

    def remote(src, dst, ssem, rsem, dev):
        return pltpu.make_async_remote_copy(
            src_ref=src, dst_ref=dst, send_sem=ssem, recv_sem=rsem, device_id=dev, device_id_type=MESH
        )

    def point_copy(h, d, slot):
        return remote(sendbuf[h].at[d], recvbuf[h].at[slot], p_send.at[h, d], p_recv.at[h, slot], at(d))

    def target_copy(d, slot):
        return remote(tsend.at[d], trecv.at[slot], t_send.at[d], t_recv.at[slot], at(d))

    def dist_copy(d, slot):
        return remote(dsend.at[d], dret.at[slot], d_send.at[d], d_recv.at[slot], at(d))

    def count_copy(z2, slot):
        return remote(csend.at[z2], crecv.at[slot], c_send.at[z2], c_recv.at[slot], (x, c, z2, y))

    def fresh_copy(g2, slot):
        return remote(fsend.at[g2], frecv.at[slot], f_send.at[g2], f_recv.at[slot], (g2 // nc, g2 % nc, z, y))

    def others(n, own, fn):
        def body(i, _):
            @pl.when(i != own)
            def _():
                fn(i)

            return 0

        lax.fori_loop(0, n, body, 0)

    def offset(i):
        turn = (2 * ((i + 2 * c) % nx) + 1) % 5 if nx == 4 else i % nx
        return turn, i // nx

    barrier = pltpu.get_barrier_semaphore()
    others(slab, me, lambda d: pl.semaphore_signal(barrier, inc=1, device_id=at(d), device_id_type=MESH))
    others(
        NZ, z, lambda z2: pl.semaphore_signal(barrier, inc=1, device_id=(x, c, z2, y), device_id_type=MESH)
    )
    own_copy = pltpu.make_async_copy(
        centroids.at[pl.ds(pl.multiple_of(g * BS, BS), BS)], table.at[z], local_sem
    )
    own_copy.start()
    points_copy = pltpu.make_async_copy(points_in, points, points_sem)
    points_copy.start()

    ids = blocks_row[...]
    dest = ((ids & (ng - 1)) * ny + (lax.shift_right_logical(ids, ng.bit_length() - 1) & (ny - 1))) * NZ
    dest = dest + lax.shift_right_logical(ids, (ng * ny).bit_length() - 1)
    strip = min(256, npoints)
    earlier = lax.broadcasted_iota(jnp.int32, (strip, strip), 0) < lax.broadcasted_iota(jnp.int32, (strip, strip), 1)
    earlier = jnp.where(earlier, 1.0, 0.0).astype(BF16)
    strips = [dest[:, q * strip : (q + 1) * strip] for q in range(npoints // strip)]
    members = [
        jnp.where(lax.broadcasted_iota(jnp.int32, (slab * NZ, strip), 0) == part, 1.0, 0.0) for part in strips
    ]
    seen = jnp.zeros((slab * NZ, 1), F32)
    ranks = []
    for member in members:
        before = jnp.dot(member.astype(BF16), earlier, preferred_element_type=F32) + seen
        ranks.append(jnp.sum(member * before, axis=0, keepdims=True))
        seen = seen + jnp.sum(member, axis=1, keepdims=True)
    rank = jnp.concatenate(ranks, axis=1).astype(jnp.int32)
    slots = dest * DEPTH + rank
    slots_row[...] = slots
    slots_col[...] = jnp.broadcast_to(slots.astype(F32), (128, npoints)).T.astype(jnp.int32)

    value = (finals_row[...] + 1).astype(F32)
    which = lax.broadcasted_iota(jnp.int32, (slab * NZ, npoints), 0) == dest
    place = lax.broadcasted_iota(jnp.int32, (128, npoints), 0) == rank + (me % per) * DEPTH
    tiles = lax.dot_general(
        jnp.where(which, value, 0.0).astype(BF16), jnp.where(place, 1.0, 0.0).astype(BF16), NT,
        preferred_element_type=F32,
    )
    tsend[...] = tiles.reshape(slab, NZ, 128)
    trecv[me] = tsend[me]
    own_copy.wait()
    pl.semaphore_wait(barrier, slab - 1 + NZ - 1)
    others(slab, me, lambda d: target_copy(d, me).start())

    def ring_copy(way, step, back):
        step_z = 1 if way == 0 else -1
        owner = (z - step_z * (step - back) + 2 * NZ) % NZ if not back else (z - step_z * (step + 1) + 2 * NZ) % NZ
        rows = slice(None) if step < 3 else pl.ds(way * (BS // 2), BS // 2)
        ref = table.at[owner, rows] if step == 3 else table.at[owner]
        return remote(ref, ref, g_send.at[way, step], g_recv.at[way, step], along(step_z))

    def ring_step(step):
        for way in range(2):
            if step:
                ring_copy(way, step - 1, 1).wait_recv()
            if step < 4:
                ring_copy(way, step, 0).start()

    ring_step(0)
    points_copy.wait()

    def dispatch(h):
        def body(i, _):
            dx, dc = offset(i)
            g2 = ((x + dx) % nx) * nc + (c + dc) % nc
            hot = lax.broadcasted_iota(jnp.int32, (ny * chunk, npoints), 0) + g2 * (ny * chunk) == slots_row[...]
            moved = jnp.dot(
                jnp.where(hot, 1.0, 0.0).astype(BF16), points[:, pieces[h]],
                preferred_element_type=F32,
            ).astype(BF16)
            sendbuf[h][pl.ds(g2 * ny, ny)] = moved.reshape(ny, chunk, moved.shape[1])
            for dy in range(ny):
                d = g2 * ny + (y + dy) % ny

                @pl.when(d != me)
                def _():
                    point_copy(h, d, me).start()

            return 0

        lax.fori_loop(0, ng, body, 0)
        recvbuf[h][me] = sendbuf[h][me]

    for h in range(len(pieces)):
        dispatch(h)
        ring_step(h + 1)
    for step in range(len(pieces) + 1, 5):
        ring_step(step)

    others(slab, me, lambda s: target_copy(s, s).wait_recv())
    for q in range(max(1, slab // per)):
        tile = trecv[q * per]
        for s in range(q * per + 1, min(slab, (q + 1) * per)):
            tile = tile + trecv[s]
        tall[:, q * 128 : (q + 1) * 128] = tile

    def norms(j, _):
        block = table[j].astype(F32)
        column = jnp.sum(block * block, axis=1, keepdims=True)
        cnorm[j] = jnp.broadcast_to(column, (BS, 128)).T[:8]
        return 0

    lax.fori_loop(0, NZ, norms, 0)

    def rows_of(h, j):
        return recvbuf[h][:, pl.ds(pl.multiple_of(j * DEPTH, DEPTH), DEPTH), :].reshape(nrow, -1)

    def add_up(h):
        def body(j, _):
            want = tall[pl.ds(j, 1), :nrow]
            centroid = lax.broadcasted_iota(jnp.int32, (BS, nrow), 0).astype(F32) + 1.0
            hot = jnp.where(want == centroid, 1.0, 0.0).astype(BF16)
            sums[j, :, pieces[h]] = jnp.dot(hot, rows_of(h, j), preferred_element_type=F32)
            if h == 0:
                csend[j] = lax.dot_general(jnp.ones((8, nrow), BF16), hot, NT, preferred_element_type=F32)
            return 0

        lax.fori_loop(0, NZ, body, 0)

    def measure(h):
        def body(j, _):
            rows = rows_of(h, j)
            wide = rows.astype(F32)
            cross = lax.dot_general(
                rows, table[j, :, pieces[h]], NT, preferred_element_type=F32
            )
            part = jnp.sum(wide * wide, axis=1, keepdims=True) - 2.0 * cross
            if h > 0:
                part = part + partial[j]
            if h < len(pieces) - 1:
                partial[j] = part
            else:
                whole = (part + cnorm[j, :1, :]) / width
                dsend[:, pl.ds(pl.multiple_of(j * DEPTH, DEPTH), DEPTH), :] = whole.astype(BF16).reshape(
                    slab, DEPTH, BS
                )
            return 0

        lax.fori_loop(0, NZ, body, 0)

    half = BS // 2

    def reduce_copy(h, way, step):
        rows = pl.ds(way * half, half)
        src = rsend[h].at[way, step, rows] if step == 0 else rsend[h].at[way, step]
        dst = rrecv[h].at[way, step, rows] if step == 0 else rrecv[h].at[way, step]
        return remote(src, dst, r_send.at[h, way, step], r_recv.at[h, way, step], along(1 if way == 0 else -1))

    def reduce_step(h, step):
        piece = pieces[h]
        for way in range(2):
            lo, hi = way * half, (way + 1) * half
            if step == 0:
                rsend[h][way, 0, lo:hi] = sums[(z + 4) % NZ, lo:hi, piece].astype(BF16)
            else:
                target = (z + 4 - step) % NZ if way == 0 else (z + 4 + step) % NZ
                reduce_copy(h, way, step - 1).wait_recv()
                if step == 1:
                    olo, ohi = (1 - way) * half, (2 - way) * half
                    rsend[h][way, 1, lo:hi] = (
                        sums[target, lo:hi, piece] + rrecv[h][way, 0, lo:hi].astype(F32)
                    ).astype(BF16)
                    rsend[h][way, 1, olo:ohi] = sums[target, olo:ohi, piece].astype(BF16)
                else:
                    rsend[h][way, step] = (
                        sums[target, :, piece] + rrecv[h][way, step - 1].astype(F32)
                    ).astype(BF16)
            reduce_copy(h, way, step).start()

    def finish(h):
        piece = pieces[h]
        for way in range(2):
            reduce_copy(h, way, 3).wait_recv()
        if h == 0:
            others(NZ, z, lambda z2: count_copy(z2, z2).wait_recv())
            total = csend[z]
            crecv[z] = total
            total = crecv[0]
            for z2 in range(1, NZ):
                total = total + crecv[z2]
            denom[...] = jnp.broadcast_to(total[:1], (128, BS)).T + 1.0
        own = (
            sums[z, :, piece] + rrecv[h][0, 3].astype(F32) + rrecv[h][1, 3].astype(F32)
            + table[z, :, piece].astype(F32)
        )
        share = width // ng
        for q in range(own.shape[1] // share):
            g2 = piece.start // share + q
            fsend[g2] = (own[:, q * share : (q + 1) * share] / denom[:, :share]).astype(BF16)

            @pl.when(g2 != g)
            def _():
                fresh_copy(g2, g).start()

    def give_back(i, _):
        dx, dc = offset(i)
        g2 = ((x + dx) % nx) * nc + (c + dc) % nc
        for dy in range(ny):
            d = g2 * ny + (y + dy) % ny

            @pl.when(d != me)
            def _():
                dist_copy(d, me).start()

        return 0

    def arrived(h):
        others(slab, me, lambda s: point_copy(h, s, s).wait_recv())

    last = len(pieces) - 1
    for h in range(last):
        arrived(h)
        add_up(h)
        if h == 0:
            others(NZ, z, lambda z2: count_copy(z2, z).start())
        reduce_step(h, 0)
        measure(h)
        for step in range(1, 4 if h < last - 1 else 3):
            reduce_step(h, step)
        if h < last - 1:
            finish(h)
    arrived(last)
    measure(last)
    lax.fori_loop(0, ng, give_back, 0)
    dret[me] = dsend[me]
    add_up(last)
    reduce_step(last, 0)
    reduce_step(last - 1, 3)

    def bring(i):
        dx, dc = offset(i)
        g2 = ((x + nx - dx) % nx) * nc + (c + dc) % nc
        for dy in range(ny):
            d = g2 * ny + dy

            @pl.when(d != me)
            def _():
                dist_copy(d, d).wait_recv()

        hot = lax.broadcasted_iota(jnp.int32, (npoints, ny * chunk), 1) + g2 * (ny * chunk) == slots_col[:, :1]
        part = jnp.dot(
            jnp.where(hot, 1.0, 0.0).astype(BF16), dret[pl.ds(g2 * ny, ny)].reshape(ny * chunk, BS),
            preferred_element_type=F32,
        )

        @pl.when(i == 0)
        def _():
            acc[...] = part

        @pl.when(i > 0)
        def _():
            acc[...] += part

    def bring_some(low, high):
        def body(i, _):
            bring(i)
            return 0

        lax.fori_loop(low, high, body, 0)

    def sent(h):
        others(slab, me, lambda d: point_copy(h, d, me).wait_send())

    sent(0)
    reduce_step(last, 1)
    finish(last - 1)
    bring_some(0, ng // 4)
    for h in range(1, len(pieces)):
        sent(h)
    reduce_step(last, 2)
    others(slab, me, lambda d: target_copy(d, me).wait_send())
    others(NZ, z, lambda z2: count_copy(z2, z).wait_send())
    for way in range(2):
        for step in range(4):
            ring_copy(way, step, 0).wait_send()
    bring_some(ng // 4, ng // 2)
    reduce_step(last, 3)
    bring_some(ng // 2, 3 * ng // 4)
    finish(last)
    for h in range(len(pieces)):
        for way in range(2):
            for step in range(4):
                reduce_copy(h, way, step).wait_send()
    bring_some(3 * ng // 4, ng)
    near[...] = acc[...].astype(BF16)
    out_copy = pltpu.make_async_copy(near, dist_out, points_sem)
    out_copy.start()

    others(ng, g, lambda g2: fresh_copy(g2, g2).wait_recv())
    frecv[g] = fsend[g]
    others(slab, me, lambda d: dist_copy(d, me).wait_send())
    others(ng, g, lambda g2: fresh_copy(g2, g).wait_send())
    out_copy.wait()


def bounds(width):
    edges = [0]
    for part in SPLIT:
        edges.append(edges[-1] + part * width // sum(SPLIT))
    return list(zip(edges[:-1], edges[1:]))


def fused(blocks, finals, points, centroids, dims):
    nx, nc, ny = dims
    ng, slab = nx * nc, nx * nc * ny
    npoints, width = points.shape
    chunk, share = NZ * DEPTH, width // (nx * nc)
    sizes = [b - a for a, b in bounds(width)]
    n = len(sizes)
    vmem, dma = pltpu.VMEM, pltpu.SemaphoreType.DMA
    tall_lanes = max(1, slab * DEPTH // 128) * 128
    return pl.pallas_call(
        functools.partial(kernel, dims),
        out_shape=(
            jax.ShapeDtypeStruct((npoints, BS), BF16),
            jax.ShapeDtypeStruct((ng, BS, share), BF16),
        ),
        in_specs=[pl.BlockSpec(memory_space=vmem)] * 2 + [pl.BlockSpec(memory_space=pl.ANY)] * 2,
        out_specs=(pl.BlockSpec(memory_space=pl.ANY), pl.BlockSpec(memory_space=vmem)),
        scratch_shapes=[
            vmem((npoints, width), BF16),
            tuple(vmem((slab, chunk, size), BF16) for size in sizes),
            tuple(vmem((slab, chunk, size), BF16) for size in sizes),
            tuple(vmem((2, 4, BS, size), BF16) for size in sizes),
            tuple(vmem((2, 4, BS, size), BF16) for size in sizes),
            vmem((NZ, BS, width), BF16),
            vmem((NZ, BS, width), F32),
            vmem((NZ, slab * DEPTH, BS), F32),
            vmem((slab, chunk, BS), BF16),
            vmem((slab, chunk, BS), BF16),
            vmem((slab, NZ, 128), F32),
            vmem((slab, NZ, 128), F32),
            vmem((NZ, tall_lanes), F32),
            vmem((NZ, 8, BS), F32),
            vmem((NZ, 8, BS), F32),
            vmem((NZ, 8, BS), F32),
            vmem((BS, 128), F32),
            vmem((ng, BS, share), BF16),
            vmem((npoints, BS), F32),
            vmem((npoints, BS), BF16),
            vmem((1, npoints), jnp.int32),
            vmem((npoints, 128), jnp.int32),
            dma((n, slab)), dma((n, slab)), dma((slab,)), dma((slab,)), dma((slab,)), dma((slab,)),
            dma((2, 4)), dma((2, 4)), dma((n, 2, 4)), dma((n, 2, 4)),
            dma((NZ,)), dma((NZ,)), dma((ng,)), dma((ng,)), dma, dma,
        ],
        compiler_params=pltpu.CompilerParams(
            collective_id=0, has_side_effects=True, vmem_limit_bytes=67043328
        ),
    )(blocks.reshape(1, npoints), finals[None, :], points, centroids)


def shards(points, blocks, finals, centroids):
    dims = tuple(lax.axis_size(a) for a in ("x", "core", "y"))
    distances, refreshed = fused(blocks, finals, points, centroids, dims)
    return distances, refreshed.reshape(-1, refreshed.shape[2]).astype(F32)


def solution(mesh):
    ngrp, ndev = mesh.shape["grp"], mesh.shape["dev"]
    fine = Mesh(mesh.devices.reshape(ngrp // 2, 2, NZ, ndev // NZ), ("x", "core", "z", "y"))
    rows = ("x", "core", "z", "y")
    return jax.shard_map(
        shards,
        mesh=fine,
        in_specs=(P(rows, None), P(rows, None), P(rows), P(("z", "y"), None)),
        out_specs=(P(rows, None), P(("z", "y"), ("x", "core"))),
        check_vma=False,
    )
```
